8 devices in a mesh: dp: 2 (over z, y), stage: 2 (over x), tp: 2 (over core).
Axes of the slice: x: 2, y: 2, z: 1, core: 2. Of those that a mesh axis runs over, the one named last changes fastest.
Arguments:
- act_in: bfloat16 [2, 4, 28, 28, 1024], P('stage', ('dp', 'tp'))
- w_conv: bfloat16 [2, 3, 3, 1024, 1024], P('stage', None, None, 'tp')
- w_short: bfloat16 [2, 1024, 1024], P('stage', 'tp')
- gamma: float32 [2, 1024], P('stage', 'tp')
- beta: float32 [2, 1024], P('stage', 'tp')
- gamma_s: float32 [2, 1024], P('stage', 'tp')
- grad_z: bfloat16 [2, 4, 28, 28, 1024], P('stage', 'dp', None, None, 'tp')
Outputs:
- output 1: bfloat16 [2, 4, 28, 28, 1024], P('stage', 'dp', None, None, 'tp')
- output 2: bfloat16 [2, 4, 28, 28, 1024], P('stage', ('dp', 'tp'))
- output 3: float32 [2, 3, 3, 1024, 1024], P('stage', None, None, 'tp')
- output 4: float32 [2, 1024, 1024], P('stage', 'tp')
All inputs are finite; a program needn't handle non-finite values.
Results may differ from the reference program's by a relative error of at most 0.0027.
Values are sent between devices in bfloat16 or wider.
A program may use at most 1 GiB of HBM per device.

```python
import jax
import jax.numpy as jnp
from jax import lax

NUM_STAGES = 2
BATCH_ALL = 4
BLOCK_IMGS = 1
IMG_HEIGHT = 28
IMG_WIDTH = 28
CH_IN = 1024
CH_OUT = 1024


def place_slot(array_in, slot_index):
    pad_before = jnp.zeros((slot_index,) + array_in.shape, array_in.dtype)
    pad_after = jnp.zeros((NUM_STAGES - slot_index - 1,) + array_in.shape, array_in.dtype)
    return jnp.concatenate([pad_before, array_in[None], pad_after], axis=0)


def setup_inputs(seed: int = 0) -> dict:
    key_list = jax.random.split(jax.random.key(seed), 7)
    act_draw = jax.random.normal(key_list[0], (BATCH_ALL, IMG_HEIGHT, IMG_WIDTH, CH_IN), jnp.float32)
    conv_draw = jax.random.normal(key_list[1], (3, 3, CH_IN, CH_OUT), jnp.float32) * (9 * CH_IN) ** -0.5
    short_draw = jax.random.normal(key_list[2], (CH_IN, CH_OUT), jnp.float32) * CH_IN ** -0.5
    gamma_draw = jax.random.uniform(key_list[3], (CH_OUT,), jnp.float32, 0.5, 1.5)
    beta_draw = 0.5 * jax.random.normal(key_list[4], (CH_OUT,), jnp.float32)
    gamma_s_draw = jax.random.uniform(key_list[5], (CH_OUT,), jnp.float32, 0.5, 1.5)
    grad_draw = jax.random.normal(key_list[6], (BATCH_ALL, IMG_HEIGHT, IMG_WIDTH, CH_OUT), jnp.float32)
    return {
        "act_in": place_slot(act_draw.astype(jnp.bfloat16), 0),
        "w_conv": place_slot(conv_draw.astype(jnp.bfloat16), 1),
        "w_short": place_slot(short_draw.astype(jnp.bfloat16), 1),
        "gamma": place_slot(gamma_draw, 1),
        "beta": place_slot(beta_draw, 1),
        "gamma_s": place_slot(gamma_s_draw, 1),
        "grad_z": place_slot(grad_draw.astype(jnp.bfloat16), 1),
    }


def reference(act_in, w_conv, w_short, gamma, beta, gamma_s, grad_z):
    kernel = w_conv[1].astype(jnp.float32)
    short_w = w_short[1].astype(jnp.float32)
    scale_main = gamma[1]
    shift_main = beta[1]
    scale_short = gamma_s[1]
    num_blocks = BATCH_ALL // BLOCK_IMGS
    act_blocks = act_in[0].reshape(num_blocks, BLOCK_IMGS, IMG_HEIGHT, IMG_WIDTH, CH_IN)
    grad_blocks = grad_z[1].reshape(num_blocks, BLOCK_IMGS, IMG_HEIGHT, IMG_WIDTH, CH_OUT)

    def linear_part(images, conv_w, proj_w):
        pre_act = lax.conv_general_dilated(images, conv_w, (1, 1), "SAME", dimension_numbers=("NHWC", "HWIO", "NHWC"))
        short_out = jnp.einsum("nhwc,co->nhwo", images, proj_w)
        return pre_act, short_out

    def block_step(acc_pair, block_in):
        act_blk, grad_blk = block_in
        (pre_act, short_out), pull_back = jax.vjp(linear_part, act_blk.astype(jnp.float32), kernel, short_w)
        mixed_sum = pre_act * scale_main + shift_main + short_out * scale_short
        z_blk = jnp.maximum(mixed_sum, 0.0).astype(jnp.bfloat16)
        mask_pos = mixed_sum > 0.0
        grad_wide = grad_blk.astype(jnp.float32)
        g_main = jnp.where(mask_pos, grad_wide * scale_main, 0.0).astype(jnp.bfloat16)
        g_short = jnp.where(mask_pos, grad_wide * scale_short, 0.0).astype(jnp.bfloat16)
        grad_images, grad_conv, grad_proj = pull_back((g_main.astype(jnp.float32), g_short.astype(jnp.float32)))
        new_acc = (acc_pair[0] + grad_conv, acc_pair[1] + grad_proj)
        return new_acc, (z_blk, grad_images.astype(jnp.bfloat16))

    acc_init = (jnp.zeros((3, 3, CH_IN, CH_OUT), jnp.float32), jnp.zeros((CH_IN, CH_OUT), jnp.float32))
    (dw_sum, dws_sum), (z_blocks, dx_blocks) = lax.scan(block_step, acc_init, (act_blocks, grad_blocks))
    z_all = z_blocks.reshape(BATCH_ALL, IMG_HEIGHT, IMG_WIDTH, CH_OUT)
    dx_all = dx_blocks.reshape(BATCH_ALL, IMG_HEIGHT, IMG_WIDTH, CH_IN)
    return (place_slot(z_all, 1), place_slot(dx_all, 0), place_slot(dw_sum, 1), place_slot(dws_sum, 1))
```

```python
import functools

import jax
import jax.numpy as jnp
from jax import lax
from jax.experimental import pallas as pl
from jax.experimental.pallas import tpu as pltpu
from jax.sharding import PartitionSpec as P


SIDE = 28
LO = 7
GRP = 16
HAL = LO + 2
GROUPS = HAL * HAL + LO * LO
PIX = SIDE * SIDE
HALF = 512
CH = 1024
TILE = 256
F32 = jnp.float32
BF16 = jnp.bfloat16
VMEM_LIMIT = 60 * 1024 * 1024


def params(n_axes):
    return pltpu.CompilerParams(dimension_semantics=("arbitrary",) * n_axes, vmem_limit_bytes=VMEM_LIMIT)


def cost(flops, bytes_accessed):
    return pl.CostEstimate(flops=int(flops), bytes_accessed=int(bytes_accessed), transcendentals=0)


def order_matrix(transposed):
    shape = (128, 112) if transposed else (112, 128)
    row = lax.broadcasted_iota(jnp.int32, shape, 1 if transposed else 0)
    col = lax.broadcasted_iota(jnp.int32, shape, 0 if transposed else 1)
    w_lo, h_hi, w_hi = row // 16, (row // 4) % 4, row % 4
    return (col == h_hi * 32 + w_hi * 7 + w_lo).astype(F32).astype(BF16)


def to_blocks_kernel(t_ref, img_ref, own_ref, peer_ref, *rest):
    pad_ref = rest[-1]
    pad_ref[...] = jnp.zeros_like(pad_ref)
    pad_ref[:, :SIDE, :] = img_ref[...]
    select = order_matrix(False)
    step = pl.program_id(0)
    for lo in range(LO):
        rows = jnp.concatenate([pad_ref[hi * LO + lo] for hi in range(4)], axis=0)
        out = jnp.dot(select, rows, preferred_element_type=F32).astype(BF16)
        part = slice(lo * 112, (lo + 1) * 112)

        @pl.when(step == 0)
        def _():
            own_ref[part, :] = out

        @pl.when(step == 1)
        def _():
            peer_ref[part, :] = out

        if len(rest) > 1:
            rest[0][part, :] = out


def to_blocks(me, array, in_map, joined):
    plane = pl.BlockSpec((PIX, HALF), lambda k, t: (0, 0))
    return pl.pallas_call(
        to_blocks_kernel,
        grid_spec=pltpu.PrefetchScalarGridSpec(
            num_scalar_prefetch=1,
            grid=(2,),
            in_specs=[pl.BlockSpec((None, None, SIDE, SIDE, HALF), in_map)],
            out_specs=[plane, plane] + ([pl.BlockSpec((PIX, HALF), lambda k, t: (0, k))] if joined else []),
            scratch_shapes=[pltpu.VMEM((SIDE, 32, HALF), BF16)],
        ),
        out_shape=[jax.ShapeDtypeStruct((PIX, HALF), BF16)] * 2
        + ([jax.ShapeDtypeStruct((PIX, CH), BF16)] if joined else []),
        compiler_params=params(1),
        cost_estimate=cost(2 * 2 * 7 * 112 * 128 * HALF * 2, 2 * 2 * PIX * HALF * 2),
        name="to_blocks",
    )(me, array)


def from_blocks_kernel(idx_ref, z_ref, z_near_ref, dx_own_ref, dx_peer_ref, z_out, dx_out):
    select = order_matrix(True)
    step = pl.program_id(0)
    stage = idx_ref[1]

    def emit(ref, out_ref):
        for lo in range(LO):
            rows = jnp.dot(select, ref[lo * 112:(lo + 1) * 112, :], preferred_element_type=F32).astype(BF16)
            for hi in range(4):
                out_ref[hi * LO + lo] = rows[hi * 32:hi * 32 + SIDE, :]

    @pl.when(stage == 0)
    def _():
        z_out[...] = jnp.zeros_like(z_out)

        @pl.when(step == 0)
        def _():
            emit(dx_own_ref, dx_out)

        @pl.when(step == 1)
        def _():
            emit(dx_peer_ref, dx_out)

    @pl.when(stage == 1)
    def _():
        dx_out[...] = jnp.zeros_like(dx_out)

        @pl.when(step == 0)
        def _():
            emit(z_ref, z_out)

        @pl.when(step == 1)
        def _():
            emit(z_near_ref, z_out)


def from_blocks(idx, z, z_near, dx_own, dx_peer):
    return pl.pallas_call(
        from_blocks_kernel,
        grid_spec=pltpu.PrefetchScalarGridSpec(
            num_scalar_prefetch=1,
            grid=(2,),
            in_specs=[
                pl.BlockSpec((PIX, HALF), lambda k, m: (0, 0)),
                pl.BlockSpec((PIX, HALF), lambda k, m: (0, 1)),
                pl.BlockSpec((PIX, HALF), lambda k, m: (0, 0)),
                pl.BlockSpec((PIX, HALF), lambda k, m: (0, 0)),
            ],
            out_specs=[
                pl.BlockSpec((None, None, SIDE, SIDE, HALF), lambda k, m: (0, (m[0] + k) % 2, 0, 0, 0)),
                pl.BlockSpec((None, None, SIDE, SIDE, HALF), lambda k, m: (0, 0, 0, 0, (m[0] + k) % 2)),
            ],
        ),
        out_shape=[
            jax.ShapeDtypeStruct((1, 2, SIDE, SIDE, HALF), BF16),
            jax.ShapeDtypeStruct((1, 1, SIDE, SIDE, CH), BF16),
        ],
        compiler_params=params(1),
        cost_estimate=cost(2 * 2 * 7 * 112 * 128 * HALF * 2, 4 * 2 * PIX * HALF * 2),
        name="from_blocks",
    )(idx, z, z_near, dx_own, dx_peer)


def moved(tile, step_h, step_w):
    wide = tile.astype(F32)
    n = wide.shape[1]
    if step_h < 0:
        wide = jnp.concatenate([jnp.zeros((4, n), F32), wide[:12]], axis=0)
    if step_h > 0:
        wide = jnp.concatenate([wide[4:], jnp.zeros((4, n), F32)], axis=0)
    if step_w:
        w_hi = lax.broadcasted_iota(jnp.int32, (GRP, n), 0) % 4
        if step_w < 0:
            wide = jnp.concatenate([wide[15:], wide[:15]], axis=0)
            wide = jnp.where(w_hi == 0, 0.0, wide)
        else:
            wide = jnp.concatenate([wide[1:], wide[:1]], axis=0)
            wide = jnp.where(w_hi == 3, 0.0, wide)
    return wide.astype(BF16)


def fill_halo(dst_ref, value):
    n = value.shape[1]
    groups = value.reshape(LO, LO, GRP, n)
    for a in range(HAL):
        step_h = -1 if a == 0 else (1 if a == HAL - 1 else 0)
        if not step_h:
            dst_ref[a * HAL + 1:a * HAL + 1 + LO] = groups[a - 1]
        for b in range(HAL):
            step_w = -1 if b == 0 else (1 if b == HAL - 1 else 0)
            if step_h or step_w:
                dst_ref[a * HAL + b] = moved(groups[(a - 1) % LO, (b - 1) % LO], step_h, step_w)


def window(ref, i, j):
    parts = [ref[pl.ds((i + a) * HAL + j, LO)] for a in range(LO)]
    whole = jnp.concatenate(parts, axis=0)
    return whole.reshape(PIX, whole.shape[-1])


def forward_sums(xh_ref, w_ref, s_ref, pre, short):
    for i in range(3):
        for j in range(3):
            term = jnp.dot(window(xh_ref, i, j), w_ref[i * 3 + j], preferred_element_type=F32)
            pre = term if pre is None else pre + term
    term = jnp.dot(window(xh_ref, 1, 1), s_ref[...], preferred_element_type=F32)
    return pre, term if short is None else short + term


def fwd_first_kernel(x_ref, w_ref, s_ref, pre_ref, short_ref, xh_ref):
    @pl.when(pl.program_id(0) == 0)
    def _():
        fill_halo(xh_ref, x_ref[...])

    pre_ref[...], short_ref[...] = forward_sums(xh_ref, w_ref, s_ref, None, None)


def fwd_last_kernel(t_ref, x_ref, w_ref, s_ref, pre_ref, short_ref, vec_ref, dza_ref, dzb_ref, z_ref, dzm_ref, g_ref, xh_ref):
    @pl.when(pl.program_id(0) == 0)
    def _():
        fill_halo(xh_ref, x_ref[...])

    pre, short = forward_sums(xh_ref, w_ref, s_ref, pre_ref[...], short_ref[...])
    u = pre * vec_ref[0:1, :] + vec_ref[1:2, :] + short * vec_ref[2:3, :]
    z_ref[...] = jnp.maximum(u, 0.0).astype(BF16)
    mine = pl.program_id(0) // 2 == t_ref[0]
    dz = jnp.where(mine, dza_ref[...].astype(F32), dzb_ref[...].astype(F32))
    dz = jnp.where(u > 0.0, dz, 0.0)
    dzm_ref[...] = dz.astype(BF16)
    both_grads(dz, vec_ref, g_ref)


def both_grads(dz, vec_ref, g_ref):
    g_ref[HAL * HAL:] = (dz * vec_ref[2:3, :]).astype(BF16).reshape(LO * LO, GRP, -1)
    fill_halo(g_ref, (dz * vec_ref[0:1, :]).astype(BF16))


FWD_FLOPS = 2 * PIX * HALF * CH * 10
W_BYTES = 10 * HALF * CH * 2


def fwd_first(x, w, s):
    return pl.pallas_call(
        fwd_first_kernel,
        grid=(CH // TILE,),
        in_specs=[
            pl.BlockSpec((PIX, HALF), lambda j: (0, 0)),
            pl.BlockSpec((9, HALF, TILE), lambda j: (0, 0, j)),
            pl.BlockSpec((HALF, TILE), lambda j: (0, j)),
        ],
        out_specs=[pl.BlockSpec((PIX, TILE), lambda j: (0, j))] * 2,
        out_shape=[jax.ShapeDtypeStruct((PIX, CH), F32)] * 2,
        scratch_shapes=[pltpu.VMEM((HAL * HAL, GRP, HALF), BF16)],
        compiler_params=params(1),
        cost_estimate=cost(FWD_FLOPS, W_BYTES),
        name="fwd_first",
    )(x, w, s)


def fwd_last(me, x, w, s, pre, short, vec, dz_own, dz_peer):
    tile = pl.BlockSpec((PIX, TILE), lambda j, t: (0, j))
    return pl.pallas_call(
        fwd_last_kernel,
        grid_spec=pltpu.PrefetchScalarGridSpec(
            num_scalar_prefetch=1,
            grid=(CH // TILE,),
            in_specs=[
                pl.BlockSpec((PIX, HALF), lambda j, t: (0, 0)),
                pl.BlockSpec((9, HALF, TILE), lambda j, t: (0, 0, j)),
                pl.BlockSpec((HALF, TILE), lambda j, t: (0, j)),
                tile,
                tile,
                pl.BlockSpec((3, TILE), lambda j, t: (0, j)),
                pl.BlockSpec((PIX, TILE), lambda j, t: (0, jnp.where(j // 2 == t[0], j % 2, 1 - t[0]))),
                pl.BlockSpec((PIX, TILE), lambda j, t: (0, jnp.where(j // 2 == t[0], t[0], j % 2))),
            ],
            out_specs=[
                pl.BlockSpec((PIX, TILE), lambda j, t: (0, (j + 2 * t[0]) % 4)),
                tile,
                pl.BlockSpec((GROUPS, GRP, TILE), lambda j, t: (0, 0, j)),
            ],
            scratch_shapes=[pltpu.VMEM((HAL * HAL, GRP, HALF), BF16)],
        ),
        out_shape=[
            jax.ShapeDtypeStruct((PIX, CH), BF16),
            jax.ShapeDtypeStruct((PIX, CH), BF16),
            jax.ShapeDtypeStruct((GROUPS, GRP, CH), BF16),
        ],
        compiler_params=params(1),
        cost_estimate=cost(FWD_FLOPS, W_BYTES),
        name="fwd_last",
    )(me, x, w, s, pre, short, vec, dz_own, dz_peer)


def grads_kernel(dzm_ref, vec_ref, g_ref):
    both_grads(dzm_ref[...].astype(F32), vec_ref, g_ref)


def grads(dzm, vec):
    return pl.pallas_call(
        grads_kernel,
        grid=(CH // TILE,),
        in_specs=[pl.BlockSpec((PIX, TILE), lambda j: (0, j)), pl.BlockSpec((3, TILE), lambda j: (0, j))],
        out_specs=pl.BlockSpec((GROUPS, GRP, TILE), lambda j: (0, 0, j)),
        out_shape=jax.ShapeDtypeStruct((GROUPS, GRP, CH), BF16),
        compiler_params=params(1),
        cost_estimate=cost(8 * PIX * CH, 8 * PIX * CH),
        name="grads",
    )(dzm, vec)


def dot_nt(a, b):
    return lax.dot_general(a, b, (((1,), (1,)), ((), ())), preferred_element_type=F32)


def dx_kernel(gh_ref, w_ref, s_ref, dx_ref):
    total = dot_nt(gh_ref[HAL * HAL:].reshape(PIX, CH), s_ref[...])
    for i in range(3):
        for j in range(3):
            total = total + dot_nt(window(gh_ref, 2 - i, 2 - j), w_ref[i * 3 + j])
    dx_ref[...] = total.astype(BF16)


def dx_half(g, w, s):
    return pl.pallas_call(
        dx_kernel,
        grid=(HALF // TILE,),
        in_specs=[
            pl.BlockSpec((GROUPS, GRP, CH), lambda j: (0, 0, 0)),
            pl.BlockSpec((9, TILE, CH), lambda j: (0, j, 0)),
            pl.BlockSpec((TILE, CH), lambda j: (j, 0)),
        ],
        out_specs=pl.BlockSpec((PIX, TILE), lambda j: (0, j)),
        out_shape=jax.ShapeDtypeStruct((PIX, HALF), BF16),
        compiler_params=params(1),
        cost_estimate=cost(FWD_FLOPS, W_BYTES),
        name="dx_half",
    )(g, w, s)


MAIN = 768


def dw_kernel(first, *refs):
    if first:
        xa_ref, xb_ref, ga_ref, gb_ref, dw_ref, ds_ref, xt_ref = refs
    else:
        xa_ref, xb_ref, ga_ref, gb_ref = refs[:4]
        x_tails, g_tails = refs[4:6], (refs[6:10], refs[10:14])
        dw_in, ds_in, dw_ref, ds_ref, xt_ref = refs[14:]
    step = pl.program_id(0)

    @pl.when(step == 0)
    def _():
        xt_ref[:, :MAIN] = xa_ref[:MAIN, :].T
        xt_ref[:, MAIN:2 * MAIN] = xb_ref[:MAIN, :].T
        if not first:
            ends = [xa_ref[MAIN:, :], xb_ref[MAIN:, :]] + [ref[...] for ref in x_tails]
            xt_ref[:, 2 * MAIN:] = jnp.concatenate(ends, axis=0).T

    def product(a, b, tails):
        parts = [a[:MAIN], b[:MAIN]]
        if not first:
            parts += [a[MAIN:], b[MAIN:]] + tails
        return jnp.dot(xt_ref[...], jnp.concatenate(parts, axis=0), preferred_element_type=F32)

    @pl.when(step < 9)
    def _():
        i, j = 2 - step // 3, 2 - step % 3
        tails = []
        if not first:
            for rows in g_tails:
                tail = rows[0][j]
                tail = jnp.where(i == 1, rows[1][j], tail)
                tails.append(jnp.where(i == 2, rows[2][j], tail))
        total = product(window(ga_ref, i, j), window(gb_ref, i, j), tails)
        dw_ref[...] = total if first else total + dw_in[...]

    @pl.when(step == 9)
    def _():
        tails = [] if first else [rows[3][0] for rows in g_tails]
        total = product(ga_ref[HAL * HAL:].reshape(PIX, -1), gb_ref[HAL * HAL:].reshape(PIX, -1), tails)
        ds_ref[...] = total if first else total + ds_in[...]


def weight_sums(xa, xb, b_col, ga, gb, tails=None, partial=None):
    first = partial is None
    g_spec = pl.BlockSpec((GROUPS, GRP, CH), lambda s: (0, 0, 0))
    dw_spec = pl.BlockSpec((None, None, None, HALF, CH), lambda s: (0, jnp.minimum(s, 8) // 3, jnp.minimum(s, 8) % 3, 0, 0))
    ds_spec = pl.BlockSpec((None, HALF, CH), lambda s: (0, 0, 0))
    x_rows = MAIN if first else PIX
    in_specs = [pl.BlockSpec((x_rows, HALF), lambda s: (0, 0)), pl.BlockSpec((x_rows, HALF), lambda s: (0, b_col)), g_spec, g_spec]
    args = [xa, xb, ga, gb]
    if not first:
        x_own, x_near, g_own, g_near = tails
        in_specs += [pl.BlockSpec((GRP, HALF), lambda s: (MAIN // GRP, 0))] * 2
        args += [x_own, x_near]
        for g in (g_own, g_near):
            for row in range(3):
                in_specs.append(pl.BlockSpec((3, GRP, CH), lambda s, row=row: (20 + 3 * row, 0, 0)))
            in_specs.append(pl.BlockSpec((1, GRP, CH), lambda s: (GROUPS - 1, 0, 0)))
            args += [g] * 4
        in_specs += [dw_spec, ds_spec]
        args += list(partial)
    return pl.pallas_call(
        functools.partial(dw_kernel, first),
        grid=(10,),
        in_specs=in_specs,
        out_specs=[dw_spec, ds_spec],
        out_shape=[jax.ShapeDtypeStruct((1, 3, 3, HALF, CH), F32), jax.ShapeDtypeStruct((1, HALF, CH), F32)],
        scratch_shapes=[pltpu.VMEM((HALF, 2 * MAIN if first else 2 * PIX + 2 * GRP), BF16)],
        input_output_aliases={} if first else {14: 0, 15: 1},
        compiler_params=params(1),
        cost_estimate=cost(2 * FWD_FLOPS, 2 * W_BYTES),
        name="weight_sums",
    )(*args)


def solution(mesh):
    act_spec = P("stage", ("dp", "tp"), None, None, None)
    kernel_spec = P("stage", None, None, "tp", None)
    short_spec = P("stage", "tp", None)
    vec_spec = P("stage", "tp")
    grad_spec = P("stage", "dp", None, None, "tp")
    swap = [(0, 1), (1, 0)]

    def block(act_in, w_conv, w_short, gamma, beta, gamma_s, grad_z):
        t = lax.axis_index("tp")
        me = t.astype(jnp.int32).reshape(1)
        idx = jnp.stack([t, lax.axis_index("stage")]).astype(jnp.int32)
        w_own = w_conv.reshape(9, HALF, CH)
        s_own = w_short.reshape(HALF, CH)

        img_own, img_peer, img = to_blocks(me, act_in, lambda k, m: (0, 0, 0, 0, (m[0] + k) % 2), True)
        x_own = lax.ppermute(img_own, "stage", [(0, 1)])
        x_peer = lax.ppermute(img_peer, "stage", [(0, 1)])
        w_peer = lax.ppermute(w_own, "tp", swap)
        s_peer = lax.ppermute(s_own, "tp", swap)
        vec_own = jnp.concatenate([gamma, beta, gamma_s], axis=0)
        vec_peer = lax.ppermute(vec_own, "tp", swap)
        vec = jnp.where(t == 0, jnp.concatenate([vec_own, vec_peer], axis=1), jnp.concatenate([vec_peer, vec_own], axis=1))
        dz_own, dz_send = to_blocks(me, grad_z, lambda k, m: (0, (m[0] + k) % 2, 0, 0, 0), False)
        dz_peer = lax.ppermute(dz_send, "tp", swap)

        far = lax.ppermute(img, "dp", swap)
        x_far = lax.ppermute(far, "stage", [(0, 1)])

        pre, short = fwd_first(x_own, w_own, s_own)
        x_near = lax.ppermute(x_peer, "tp", swap)
        z, dzm, g = fwd_last(me, x_peer, w_peer, s_peer, pre, short, vec, dz_own, dz_peer)
        dzm_far = lax.ppermute(dzm, "dp", swap)
        g_near = lax.ppermute(g, "tp", swap)
        z_near = lax.ppermute(z, "tp", swap)
        dx_own = lax.ppermute(dx_half(g, w_own, s_own), "stage", [(1, 0)])
        dx_peer = lax.ppermute(dx_half(g, w_peer, s_peer), "stage", [(1, 0)])
        x_diag = lax.ppermute(x_far, "tp", swap)
        g_far = grads(dzm_far, vec)
        g_diag = lax.ppermute(g_far, "tp", swap)

        partial = weight_sums(x_own, x_near, 0, g, g_near)
        z_out, grad_act = from_blocks(idx, z, z_near, dx_own, dx_peer)
        dw, ds = weight_sums(x_far, x_diag, 1, g_far, g_diag, (x_own, x_near, g, g_near), partial)
        return z_out, grad_act, dw, ds

    return jax.shard_map(block, mesh=mesh, in_specs=(act_spec, kernel_spec, short_spec, vec_spec, vec_spec, vec_spec, grad_spec), out_specs=(grad_spec, act_spec, kernel_spec, short_spec), check_vma=False)
```

```python
import functools

import jax
import jax.numpy as jnp
from jax import lax
from jax.experimental import pallas as pl
from jax.experimental.pallas import tpu as pltpu
from jax.sharding import PartitionSpec as P


SIDE = 28
LO = 7
GRP = 16
HAL = LO + 2
GROUPS = HAL * HAL + LO * LO
PIX = SIDE * SIDE
HALF = 512
CH = 1024
TILE = 256
F32 = jnp.float32
BF16 = jnp.bfloat16
VMEM_LIMIT = 60 * 1024 * 1024


def params(n_axes):
    return pltpu.CompilerParams(dimension_semantics=("arbitrary",) * n_axes, vmem_limit_bytes=VMEM_LIMIT)


def cost(flops, bytes_accessed):
    return pl.CostEstimate(flops=int(flops), bytes_accessed=int(bytes_accessed), transcendentals=0)


def order_matrix(transposed):
    shape = (128, 112) if transposed else (112, 128)
    row = lax.broadcasted_iota(jnp.int32, shape, 1 if transposed else 0)
    col = lax.broadcasted_iota(jnp.int32, shape, 0 if transposed else 1)
    w_lo, h_hi, w_hi = row // 16, (row // 4) % 4, row % 4
    return (col == h_hi * 32 + w_hi * 7 + w_lo).astype(F32).astype(BF16)


def from_blocks_kernel(idx_ref, z_ref, z_near_ref, dx_own_ref, dx_peer_ref, z_out, dx_out):
    select = order_matrix(True)
    step = pl.program_id(0)
    stage = idx_ref[1]

    def emit(ref, out_ref):
        for lo in range(LO):
            rows = jnp.dot(select, ref[lo * 112:(lo + 1) * 112, :], preferred_element_type=F32).astype(BF16)
            for hi in range(4):
                out_ref[hi * LO + lo] = rows[hi * 32:hi * 32 + SIDE, :]

    @pl.when(stage == 0)
    def _():
        z_out[...] = jnp.zeros_like(z_out)

        @pl.when(step == 0)
        def _():
            emit(dx_own_ref, dx_out)

        @pl.when(step == 1)
        def _():
            emit(dx_peer_ref, dx_out)

    @pl.when(stage == 1)
    def _():
        dx_out[...] = jnp.zeros_like(dx_out)

        @pl.when(step == 0)
        def _():
            emit(z_ref, z_out)

        @pl.when(step == 1)
        def _():
            emit(z_near_ref, z_out)


def from_blocks(idx, z, z_near, dx_own, dx_peer):
    return pl.pallas_call(
        from_blocks_kernel,
        grid_spec=pltpu.PrefetchScalarGridSpec(
            num_scalar_prefetch=1,
            grid=(2,),
            in_specs=[
                pl.BlockSpec((PIX, HALF), lambda k, m: (0, 0)),
                pl.BlockSpec((PIX, HALF), lambda k, m: (0, 1)),
                pl.BlockSpec((PIX, HALF), lambda k, m: (0, 0)),
                pl.BlockSpec((PIX, HALF), lambda k, m: (0, 0)),
            ],
            out_specs=[
                pl.BlockSpec((None, None, SIDE, SIDE, HALF), lambda k, m: (0, (m[0] + k) % 2, 0, 0, 0)),
                pl.BlockSpec((None, None, SIDE, SIDE, HALF), lambda k, m: (0, 0, 0, 0, (m[0] + k) % 2)),
            ],
        ),
        out_shape=[
            jax.ShapeDtypeStruct((1, 2, SIDE, SIDE, HALF), BF16),
            jax.ShapeDtypeStruct((1, 1, SIDE, SIDE, CH), BF16),
        ],
        compiler_params=params(1),
        cost_estimate=cost(2 * 2 * 7 * 112 * 128 * HALF * 2, 4 * 2 * PIX * HALF * 2),
        name="from_blocks",
    )(idx, z, z_near, dx_own, dx_peer)


def moved(tile, step_h, step_w):
    wide = tile.astype(F32)
    n = wide.shape[1]
    if step_h < 0:
        wide = jnp.concatenate([jnp.zeros((4, n), F32), wide[:12]], axis=0)
    if step_h > 0:
        wide = jnp.concatenate([wide[4:], jnp.zeros((4, n), F32)], axis=0)
    if step_w:
        w_hi = lax.broadcasted_iota(jnp.int32, (GRP, n), 0) % 4
        if step_w < 0:
            wide = jnp.concatenate([wide[15:], wide[:15]], axis=0)
            wide = jnp.where(w_hi == 0, 0.0, wide)
        else:
            wide = jnp.concatenate([wide[1:], wide[:1]], axis=0)
            wide = jnp.where(w_hi == 3, 0.0, wide)
    return wide.astype(BF16)


def fill_halo(dst_ref, value):
    n = value.shape[1]
    groups = value.reshape(LO, LO, GRP, n)
    for a in range(HAL):
        step_h = -1 if a == 0 else (1 if a == HAL - 1 else 0)
        if not step_h:
            dst_ref[a * HAL + 1:a * HAL + 1 + LO] = groups[a - 1]
        for b in range(HAL):
            step_w = -1 if b == 0 else (1 if b == HAL - 1 else 0)
            if step_h or step_w:
                dst_ref[a * HAL + b] = moved(groups[(a - 1) % LO, (b - 1) % LO], step_h, step_w)


def window(ref, i, j):
    parts = [ref[pl.ds((i + a) * HAL + j, LO)] for a in range(LO)]
    whole = jnp.concatenate(parts, axis=0)
    return whole.reshape(PIX, whole.shape[-1])


def both_grads(dz, vec_ref, g_ref):
    g_ref[HAL * HAL:] = (dz * vec_ref[2:3, :]).astype(BF16).reshape(LO * LO, GRP, -1)
    fill_halo(g_ref, (dz * vec_ref[0:1, :]).astype(BF16))


FWD_FLOPS = 2 * PIX * HALF * CH * 10
W_BYTES = 10 * HALF * CH * 2


def grads_kernel(dzm_ref, vec_ref, g_ref):
    both_grads(dzm_ref[...].astype(F32), vec_ref, g_ref)


def grads(dzm, vec):
    return pl.pallas_call(
        grads_kernel,
        grid=(CH // TILE,),
        in_specs=[pl.BlockSpec((PIX, TILE), lambda j: (0, j)), pl.BlockSpec((3, TILE), lambda j: (0, j))],
        out_specs=pl.BlockSpec((GROUPS, GRP, TILE), lambda j: (0, 0, j)),
        out_shape=jax.ShapeDtypeStruct((GROUPS, GRP, CH), BF16),
        compiler_params=params(1),
        cost_estimate=cost(8 * PIX * CH, 8 * PIX * CH),
        name="grads",
    )(dzm, vec)


CHUNK = 256
N_CHUNKS = CH // CHUNK
MESH = pl.DeviceIdType.MESH


def arrange(src, pad_ref, select, dst):
    pad_ref[:, :SIDE, :] = src
    for lo in range(LO):
        rows = jnp.concatenate([pad_ref[hi * LO + lo] for hi in range(4)], axis=0)
        dst[lo * 112:(lo + 1) * 112, :] = jnp.dot(select, rows, preferred_element_type=F32).astype(BF16)


def front_kernel(
    act, grad, gam, bet, gms, w_own, s_own,
    x_own, x_near, img_far, w_peer, s_peer, vec_out, z_out, dzm_out, g_out,
    pad_c, pad_h, xs, xr, xh, im, w_buf, s_buf, pre, short, dz_own, dz_send, dz_peer, vec_peer, z_st, dzm_st, g_st,
    x_send, x_recv, far_send, far_recv, near_send, near_recv, w_send, w_recv, vec_send, vec_recv, dz_sem, dz_rsem, w_local, x_local, out_sem, vec_sem,
):
    t = lax.axis_index("tp")
    stage = lax.axis_index("stage")
    dp = lax.axis_index("dp")

    barrier = pltpu.get_barrier_semaphore()
    for target in ({"tp": 1 - t}, {"stage": 1 - stage}, {"dp": 1 - dp}):
        pl.semaphore_signal(barrier, inc=1, device_id=target, device_id_type=MESH)
    pl.semaphore_wait(barrier, 3)

    def remote(src, dst, send, recv, target):
        return pltpu.make_async_remote_copy(src_ref=src, dst_ref=dst, send_sem=send, recv_sem=recv, device_id=target, device_id_type=MESH)

    peer = {"tp": 1 - t}

    def x_copy(q):
        return remote(xs.at[q], xr.at[q], x_send.at[q], x_recv.at[q], {"stage": 1 - stage})

    def far_copy(q):
        return remote(xs.at[q], img_far.at[q], far_send.at[q], far_recv.at[q], {"dp": 1 - dp})

    def near_copy(q):
        return remote(xr.at[q], x_near.at[q - 2], near_send.at[q - 2], near_recv.at[q - 2], peer)

    def keep_copy(q):
        return pltpu.make_async_copy(xr.at[q], x_own.at[q], x_local.at[q])

    @pl.when(stage == 0)
    def _():
        pad_c[...] = jnp.zeros_like(pad_c)
        select = order_matrix(False)
        for q in range(N_CHUNKS):
            col = pl.multiple_of(lax.rem(t * HALF + q * CHUNK, CH), CHUNK)
            arrange(act[0, 0, :, :, pl.ds(col, CHUNK)], pad_c, select, xs.at[q])
            x_copy(q).start()
            far_copy(q).start()
        for q in range(N_CHUNKS):
            x_copy(q).wait_send()
            far_copy(q).wait_send()
            far_copy(q).wait_recv()

    @pl.when(stage == 1)
    def _():
        w_copy = remote(w_own, w_peer, w_send.at[0], w_recv.at[0], peer)
        s_copy = remote(s_own, s_peer, w_send.at[1], w_recv.at[1], peer)
        vec_copies = [remote(ref, vec_peer.at[k], vec_send.at[k], vec_recv.at[k], peer) for k, ref in enumerate((gam, bet, gms))]
        w_copy.start()
        s_copy.start()
        for copy in vec_copies:
            copy.start()

        def w_fetch(src_w, src_s, block, q):
            rows = pl.ds(block * CHUNK, CHUNK)
            return (
                pltpu.make_async_copy(src_w.at[:, rows], w_buf.at[q], w_local.at[q, 0]),
                pltpu.make_async_copy(src_s.at[rows], s_buf.at[q], w_local.at[q, 1]),
            )

        for q in range(2):
            for copy in w_fetch(w_own, s_own, q, q):
                copy.start()

        pad_h[...] = jnp.zeros_like(pad_h)
        select = order_matrix(False)
        arrange(grad[0, 1 - t], pad_h, select, dz_send)
        dz_copy = remote(dz_send, dz_peer, dz_sem, dz_rsem, peer)
        dz_copy.start()
        arrange(grad[0, t], pad_h, select, dz_own)

        def chunk(q, carry):
            x_copy(q).wait_recv()

            @pl.when(q < 2)
            def _():
                keep_copy(q).start()

            @pl.when(q >= 2)
            def _():
                near_copy(q).start()

            fill_halo(xh, xr[q])
            for i in range(3):
                for j in range(3):
                    k = i * 3 + j
                    im[:, k * CHUNK:(k + 1) * CHUNK] = window(xh, i, j)

            @pl.when(q == 1)
            def _():
                w_copy.wait_recv()
                s_copy.wait_recv()
                for k in range(2):
                    for copy in w_fetch(w_peer, s_peer, k, k + 2):
                        copy.start()

            for copy in w_fetch(w_own, s_own, 0, q):
                copy.wait()
            for n in range(2):
                cols = slice(n * HALF, (n + 1) * HALF)
                main = jnp.dot(im[...], w_buf[q, :, :, cols].reshape(9 * CHUNK, HALF), preferred_element_type=F32)
                side = jnp.dot(xr[q], s_buf[q, :, cols], preferred_element_type=F32)

                @pl.when(q == 0)
                def _():
                    pre[:, cols] = main
                    short[:, cols] = side

                @pl.when(q > 0)
                def _():
                    pre[:, cols] += main
                    short[:, cols] += side

            return carry

        lax.fori_loop(0, N_CHUNKS, chunk, 0)

        for copy in vec_copies:
            copy.wait_recv()
        dz_copy.wait_recv()
        outs = []
        for n in range(CH // TILE):
            half, part = n // 2, slice((n % 2) * TILE, (n % 2 + 1) * TILE)
            cols = slice(n * TILE, (n + 1) * TILE)
            mine = t == half
            gamma, beta, gamma_s = (jnp.where(mine, ref[:, part], vec_peer[k, :, part]) for k, ref in enumerate((gam, bet, gms)))
            for k, row in enumerate((gamma, beta, gamma_s)):
                vec_out[k:k + 1, cols] = row
            u = pre[:, cols] * gamma + beta + short[:, cols] * gamma_s
            z_st[:, cols] = jnp.maximum(u, 0.0).astype(BF16)
            dz = jnp.where(mine, dz_own[:, part].astype(F32), dz_peer[:, part].astype(F32))
            dz = jnp.where(u > 0.0, dz, 0.0)
            dzm_st[:, cols] = dz.astype(BF16)
            g_st[HAL * HAL:, :, cols] = (dz * gamma_s).astype(BF16).reshape(LO * LO, GRP, TILE)
            fill_halo(g_st.at[:, :, cols], (dz * gamma).astype(BF16))
            to = pl.multiple_of(lax.rem(n * TILE + t * HALF, CH), TILE)
            outs.append(pltpu.make_async_copy(z_st.at[:, cols], z_out.at[:, pl.ds(to, TILE)], out_sem.at[n, 0]))
            outs.append(pltpu.make_async_copy(dzm_st.at[:, cols], dzm_out.at[:, cols], out_sem.at[n, 1]))
            outs.append(pltpu.make_async_copy(g_st.at[:, :, cols], g_out.at[:, :, cols], out_sem.at[n, 2]))
            for copy in outs[-3:]:
                copy.start()

        for copy in outs:
            copy.wait()
        for q in range(2):
            keep_copy(q).wait()
            near_copy(q + 2).wait_send()
            near_copy(q + 2).wait_recv()
        for copy in [w_copy, s_copy, dz_copy] + vec_copies:
            copy.wait_send()


def front(act_in, grad_z, gamma, beta, gamma_s, w_own, s_own):
    vmem = pl.BlockSpec(memory_space=pltpu.VMEM)
    anywhere = pl.BlockSpec(memory_space=pl.ANY)
    dma = pltpu.SemaphoreType.DMA
    chunks = (N_CHUNKS, PIX, CHUNK)
    return pl.pallas_call(
        front_kernel,
        in_specs=[vmem] * 5 + [anywhere] * 2,
        out_specs=[anywhere] * 5 + [vmem] + [anywhere] * 3,
        out_shape=[
            jax.ShapeDtypeStruct((2, PIX, CHUNK), BF16),
            jax.ShapeDtypeStruct((2, PIX, CHUNK), BF16),
            jax.ShapeDtypeStruct(chunks, BF16),
            jax.ShapeDtypeStruct((9, HALF, CH), BF16),
            jax.ShapeDtypeStruct((HALF, CH), BF16),
            jax.ShapeDtypeStruct((3, CH), F32),
            jax.ShapeDtypeStruct((PIX, CH), BF16),
            jax.ShapeDtypeStruct((PIX, CH), BF16),
            jax.ShapeDtypeStruct((GROUPS, GRP, CH), BF16),
        ],
        scratch_shapes=[
            pltpu.VMEM((SIDE, 32, CHUNK), BF16),
            pltpu.VMEM((SIDE, 32, HALF), BF16),
            pltpu.VMEM(chunks, BF16),
            pltpu.VMEM(chunks, BF16),
            pltpu.VMEM((HAL * HAL, GRP, CHUNK), BF16),
            pltpu.VMEM((PIX, 9 * CHUNK), BF16),
            pltpu.VMEM((N_CHUNKS, 9, CHUNK, CH), BF16),
            pltpu.VMEM((N_CHUNKS, CHUNK, CH), BF16),
            pltpu.VMEM((PIX, CH), F32),
            pltpu.VMEM((PIX, CH), F32),
            pltpu.VMEM((PIX, HALF), BF16),
            pltpu.VMEM((PIX, HALF), BF16),
            pltpu.VMEM((PIX, HALF), BF16),
            pltpu.VMEM((3, 1, HALF), F32),
            pltpu.VMEM((PIX, CH), BF16),
            pltpu.VMEM((PIX, CH), BF16),
            pltpu.VMEM((GROUPS, GRP, CH), BF16),
            dma((4,)), dma((4,)), dma((4,)), dma((4,)), dma((2,)), dma((2,)), dma((2,)), dma((2,)), dma((3,)), dma((3,)),
            dma, dma, dma((4, 2)), dma((2,)), dma((4, 3)), dma((1,)),
        ],
        compiler_params=pltpu.CompilerParams(collective_id=0, has_side_effects=True, vmem_limit_bytes=66 * 1000 * 1000),
        cost_estimate=cost(2 * FWD_FLOPS, 2 * W_BYTES),
        name="front",
    )(act_in, grad_z, gamma, beta, gamma_s, w_own, s_own)


def dot_nt(a, b):
    return lax.dot_general(a, b, (((1,), (1,)), ((), ())), preferred_element_type=F32)


def dx_kernel(gh_ref, w_ref, s_ref, dx_ref):
    total = dot_nt(gh_ref[HAL * HAL:].reshape(PIX, CH), s_ref[...])
    for i in range(3):
        for j in range(3):
            total = total + dot_nt(window(gh_ref, 2 - i, 2 - j), w_ref[i * 3 + j])
    dx_ref[...] = total.astype(BF16)


def dx_half(g, w, s):
    return pl.pallas_call(
        dx_kernel,
        grid=(HALF // TILE,),
        in_specs=[
            pl.BlockSpec((GROUPS, GRP, CH), lambda j: (0, 0, 0)),
            pl.BlockSpec((9, TILE, CH), lambda j: (0, j, 0)),
            pl.BlockSpec((TILE, CH), lambda j: (j, 0)),
        ],
        out_specs=pl.BlockSpec((PIX, TILE), lambda j: (0, j)),
        out_shape=jax.ShapeDtypeStruct((PIX, HALF), BF16),
        compiler_params=params(1),
        cost_estimate=cost(FWD_FLOPS, W_BYTES),
        name="dx_half",
    )(g, w, s)


MAIN = 768


def dw_kernel(first, idx_ref, *refs):
    if first:
        xa_ref, xb_ref, ga_ref, gb_ref, dw_ref, ds_ref, xt_ref = refs
    else:
        xa_ref, xb_ref, ga_ref, gb_ref = refs[:4]
        x_tails, g_tails = refs[4:6], (refs[6:10], refs[10:14])
        dw_in, ds_in, dw_ref, ds_ref, xt_ref = refs[14:]
    step = pl.program_id(0)

    stage = idx_ref[1]

    @pl.when((step == 0) & (stage == 1))
    def _():
        for q in range(2):
            rows = slice(q * CHUNK, (q + 1) * CHUNK)
            xt_ref[rows, :MAIN] = xa_ref[q, :MAIN, :].T
            xt_ref[rows, MAIN:2 * MAIN] = xb_ref[q, :MAIN, :].T
            if not first:
                ends = [xa_ref[q, MAIN:, :], xb_ref[q, MAIN:, :]] + [ref[q] for ref in x_tails]
                xt_ref[rows, 2 * MAIN:] = jnp.concatenate(ends, axis=0).T

    @pl.when(stage == 0)
    def _():
        dw_ref[...] = jnp.zeros_like(dw_ref)
        ds_ref[...] = jnp.zeros_like(ds_ref)

    def product(a, b, tails):
        parts = [a[:MAIN], b[:MAIN]]
        if not first:
            parts += [a[MAIN:], b[MAIN:]] + tails
        return jnp.dot(xt_ref[...], jnp.concatenate(parts, axis=0), preferred_element_type=F32)

    @pl.when((step < 9) & (stage == 1))
    def _():
        i, j = 2 - step // 3, 2 - step % 3
        tails = []
        if not first:
            for rows in g_tails:
                tail = rows[0][j]
                tail = jnp.where(i == 1, rows[1][j], tail)
                tails.append(jnp.where(i == 2, rows[2][j], tail))
        total = product(window(ga_ref, i, j), window(gb_ref, i, j), tails)
        dw_ref[...] = total if first else total + dw_in[...]

    @pl.when((step == 9) & (stage == 1))
    def _():
        tails = [] if first else [rows[3][0] for rows in g_tails]
        total = product(ga_ref[HAL * HAL:].reshape(PIX, -1), gb_ref[HAL * HAL:].reshape(PIX, -1), tails)
        ds_ref[...] = total if first else total + ds_in[...]


def weight_sums(idx, xa, xb, b_col, ga, gb, tails=None, partial=None):
    first = partial is None
    g_spec = pl.BlockSpec((GROUPS, GRP, CH), lambda s, m: (0, 0, 0))
    dw_spec = pl.BlockSpec((None, None, None, HALF, CH), lambda s, m: (0, jnp.minimum(s, 8) // 3, jnp.minimum(s, 8) % 3, 0, 0))
    ds_spec = pl.BlockSpec((None, HALF, CH), lambda s, m: (0, 0, 0))
    x_rows = MAIN if first else PIX
    in_specs = [pl.BlockSpec((2, x_rows, CHUNK), lambda s, m: (0, 0, 0)), pl.BlockSpec((2, x_rows, CHUNK), lambda s, m: (b_col, 0, 0)), g_spec, g_spec]
    args = [xa, xb, ga, gb]
    if not first:
        x_own, x_near, g_own, g_near = tails
        in_specs += [pl.BlockSpec((2, GRP, CHUNK), lambda s, m: (0, MAIN // GRP, 0))] * 2
        args += [x_own, x_near]
        for g in (g_own, g_near):
            for row in range(3):
                in_specs.append(pl.BlockSpec((3, GRP, CH), lambda s, m, row=row: (20 + 3 * row, 0, 0)))
            in_specs.append(pl.BlockSpec((1, GRP, CH), lambda s, m: (GROUPS - 1, 0, 0)))
            args += [g] * 4
        in_specs += [dw_spec, ds_spec]
        args += list(partial)
    return pl.pallas_call(
        functools.partial(dw_kernel, first),
        grid_spec=pltpu.PrefetchScalarGridSpec(
            num_scalar_prefetch=1,
            grid=(10,),
            in_specs=in_specs,
            out_specs=[dw_spec, ds_spec],
            scratch_shapes=[pltpu.VMEM((HALF, 2 * MAIN if first else 2 * PIX + 2 * GRP), BF16)],
        ),
        out_shape=[jax.ShapeDtypeStruct((1, 3, 3, HALF, CH), F32), jax.ShapeDtypeStruct((1, HALF, CH), F32)],
        input_output_aliases={} if first else {15: 0, 16: 1},
        compiler_params=params(1),
        cost_estimate=cost(2 * FWD_FLOPS, 2 * W_BYTES),
        name="weight_sums",
    )(idx, *args)


def solution(mesh):
    act_spec = P("stage", ("dp", "tp"), None, None, None)
    kernel_spec = P("stage", None, None, "tp", None)
    short_spec = P("stage", "tp", None)
    vec_spec = P("stage", "tp")
    grad_spec = P("stage", "dp", None, None, "tp")
    swap = [(0, 1), (1, 0)]

    def block(act_in, w_conv, w_short, gamma, beta, gamma_s, grad_z):
        idx = jnp.stack([lax.axis_index("tp"), lax.axis_index("stage")]).astype(jnp.int32)
        w_own = w_conv.reshape(9, HALF, CH)
        s_own = w_short.reshape(HALF, CH)
        x_own, x_near, img_far, w_peer, s_peer, vec, z, dzm, g = front(act_in, grad_z, gamma, beta, gamma_s, w_own, s_own)
        x_far = lax.ppermute(img_far, "stage", [(0, 1)])
        dzm_far = lax.ppermute(dzm, "dp", swap)
        g_near = lax.ppermute(g, "tp", swap)
        z_near = lax.ppermute(z, "tp", swap)
        dx_own = lax.ppermute(dx_half(g, w_own, s_own), "stage", [(1, 0)])
        dx_peer = lax.ppermute(dx_half(g, w_peer, s_peer), "stage", [(1, 0)])
        x_diag = lax.ppermute(x_far, "tp", swap)
        g_far = grads(dzm_far, vec)
        g_diag = lax.ppermute(g_far, "tp", swap)

        partial = weight_sums(idx, x_own, x_near, 0, g, g_near)
        z_out, grad_act = from_blocks(idx, z, z_near, dx_own, dx_peer)
        dw, ds = weight_sums(idx, x_far, x_diag, 1, g_far, g_diag, (x_own, x_near, g, g_near), partial)
        return z_out, grad_act, dw, ds

    return jax.shard_map(block, mesh=mesh, in_specs=(act_spec, kernel_spec, short_spec, vec_spec, vec_spec, vec_spec, grad_spec), out_specs=(grad_spec, act_spec, kernel_spec, short_spec), check_vma=False)
```

```python
import jax
import jax.numpy as jnp
from jax import lax
from jax.experimental import pallas as pl
from jax.experimental.pallas import tpu as pltpu
from jax.sharding import PartitionSpec as P

SIDE = 28
LO = 7
GRP = 16
HAL = LO + 2
GROUPS = HAL * HAL + LO * LO
PIX = SIDE * SIDE
HALF = 512
CH = 1024
TILE = 256
CHUNK = 256
N_CHUNKS = CH // CHUNK
MAIN = 768
MESH = pl.DeviceIdType.MESH
F32 = jnp.float32
BF16 = jnp.bfloat16
VMEM_LIMIT = 60 * 1024 * 1024


def params(n_axes):
    return pltpu.CompilerParams(dimension_semantics=("arbitrary",) * n_axes, vmem_limit_bytes=VMEM_LIMIT)


def cost(flops, bytes_accessed):
    return pl.CostEstimate(flops=int(flops), bytes_accessed=int(bytes_accessed), transcendentals=0)


def order_matrix(transposed):
    shape = (128, 112) if transposed else (112, 128)
    row = lax.broadcasted_iota(jnp.int32, shape, 1 if transposed else 0)
    col = lax.broadcasted_iota(jnp.int32, shape, 0 if transposed else 1)
    w_lo, h_hi, w_hi = row // 16, (row // 4) % 4, row % 4
    return (col == h_hi * 32 + w_hi * 7 + w_lo).astype(F32).astype(BF16)


def pair_matrix(first, transposed):
    shape = (224, 224) if transposed else (112, 224)
    row = lax.broadcasted_iota(jnp.int32, shape, 1 if transposed else 0)
    col = lax.broadcasted_iota(jnp.int32, shape, 0 if transposed else 1)
    image = (row // 112 + first) % 2
    row = row % 112
    w_lo, h_hi, w_hi = row // 16, (row // 4) % 4, row % 4
    return (col == h_hi * 56 + (w_hi * 7 + w_lo) * 2 + image).astype(F32).astype(BF16)


def from_blocks_kernel(idx_ref, z_ref, z_near_ref, dx_ref, z_out, dx_out):
    stage = idx_ref[1]

    @pl.when(stage == 0)
    def _():
        z_out[...] = jnp.zeros_like(z_out)
        select = order_matrix(True)
        for lo in range(LO):
            for q in range(2):
                rows = jnp.dot(select, dx_ref[q, lo * 112:(lo + 1) * 112, :], preferred_element_type=F32).astype(BF16)
                for hi in range(4):
                    dx_out[hi * LO + lo, :, q * CHUNK:(q + 1) * CHUNK] = rows[hi * 32:hi * 32 + SIDE, :]

    @pl.when(stage == 1)
    def _():
        dx_out[...] = jnp.zeros_like(dx_out)
        select = pair_matrix(idx_ref[0], True)
        for lo in range(LO):
            part = slice(lo * 112, (lo + 1) * 112)
            both = jnp.concatenate([z_ref[part, :], z_near_ref[part, :]], axis=0)
            rows = jnp.dot(select, both, preferred_element_type=F32)
            for hi in range(4):
                z_out[hi * LO + lo] = rows[hi * 56:(hi + 1) * 56].astype(BF16).reshape(SIDE, 2, CHUNK)


def from_blocks(idx, z, z_near, dx):
    z_out, dx_out = pl.pallas_call(
        from_blocks_kernel,
        grid_spec=pltpu.PrefetchScalarGridSpec(
            num_scalar_prefetch=1,
            grid=(2,),
            in_specs=[
                pl.BlockSpec((PIX, CHUNK), lambda k, m: (0, k)),
                pl.BlockSpec((PIX, CHUNK), lambda k, m: (0, k)),
                pl.BlockSpec((2, PIX, CHUNK), lambda k, m: (k, 0, 0)),
            ],
            out_specs=[
                pl.BlockSpec((SIDE, SIDE, 2, CHUNK), lambda k, m: (0, 0, 0, k)),
                pl.BlockSpec((None, None, SIDE, SIDE, HALF), lambda k, m: (0, 0, 0, 0, (m[0] + k) % 2)),
            ],
        ),
        out_shape=[
            jax.ShapeDtypeStruct((SIDE, SIDE, 2, HALF), BF16),
            jax.ShapeDtypeStruct((1, 1, SIDE, SIDE, CH), BF16),
        ],
        compiler_params=params(1),
        cost_estimate=cost(2 * 2 * 7 * 112 * 128 * HALF * 2, 4 * 2 * PIX * HALF * 2),
        name="from_blocks",
    )(idx, z, z_near, dx)
    return jnp.transpose(z_out, (2, 0, 1, 3))[None], dx_out


def moved(tile, step_h, step_w):
    wide = tile.astype(F32)
    n = wide.shape[1]
    if step_h < 0:
        wide = jnp.concatenate([jnp.zeros((4, n), F32), wide[:12]], axis=0)
    if step_h > 0:
        wide = jnp.concatenate([wide[4:], jnp.zeros((4, n), F32)], axis=0)
    if step_w:
        w_hi = lax.broadcasted_iota(jnp.int32, (GRP, n), 0) % 4
        if step_w < 0:
            wide = jnp.concatenate([wide[15:], wide[:15]], axis=0)
            wide = jnp.where(w_hi == 0, 0.0, wide)
        else:
            wide = jnp.concatenate([wide[1:], wide[:1]], axis=0)
            wide = jnp.where(w_hi == 3, 0.0, wide)
    return wide.astype(BF16)


def fill_halo(dst_ref, value):
    n = value.shape[1]
    groups = value.reshape(LO, LO, GRP, n)
    for a in range(HAL):
        step_h = -1 if a == 0 else (1 if a == HAL - 1 else 0)
        if not step_h:
            dst_ref[a * HAL + 1:a * HAL + 1 + LO] = groups[a - 1]
        for b in range(HAL):
            step_w = -1 if b == 0 else (1 if b == HAL - 1 else 0)
            if step_h or step_w:
                dst_ref[a * HAL + b] = moved(groups[(a - 1) % LO, (b - 1) % LO], step_h, step_w)


def window(ref, i, j):
    parts = [ref[pl.ds((i + a) * HAL + j, LO)] for a in range(LO)]
    whole = jnp.concatenate(parts, axis=0)
    return whole.reshape(PIX, whole.shape[-1])


def both_grads(dz, vec_ref, g_ref):
    g_ref[HAL * HAL:] = (dz * vec_ref[2:3, :]).astype(BF16).reshape(LO * LO, GRP, -1)
    fill_halo(g_ref, (dz * vec_ref[0:1, :]).astype(BF16))


FWD_FLOPS = 2 * PIX * HALF * CH * 10
W_BYTES = 10 * HALF * CH * 2


def dot_nt(a, b):
    return lax.dot_general(a, b, (((1,), (1,)), ((), ())), preferred_element_type=F32)


def tap_rows(ref, tap):
    last = tap // 9
    base = (1 - last) * ((2 - tap // 3) * HAL + 2 - tap % 3) + last * HAL * HAL
    pitch = HAL - 2 * last
    parts = [ref[pl.ds(base + a * pitch, LO if a < LO - 1 else LO - 1)] for a in range(LO)]
    return jnp.concatenate(parts, axis=0).reshape(MAIN, CH)


def main_kernel(
    act, grad, gam, bet, gms, w_own, s_own,
    x_far, x_diag, x_tails, w_peer, s_peer, vec_out, z_out, z_near, dzm_far, dzm_diag, g_tails, dx_in, sums,
    act_in, pad, xs, xr, xn, xh, im, w_buf, s_buf, pre, short, grad_in, dz_own, dz_send, dz_peer, vec_peer, z_st, dzm_st, g_st, g_near,
    act_sem, x_sem, far_sem, hop_sem, near_sem, diag_sem, w_sem, vec_sem, peer_sem, dzm_sem, dx_sem, w_local, keep_sem, tail_sem, out_sem, sum_sem,
):
    t = lax.axis_index("tp")
    stage = lax.axis_index("stage")
    dp = lax.axis_index("dp")

    def act_copy(q):
        col = pl.multiple_of(lax.rem(t * HALF + q * CHUNK, CH), CHUNK)
        return pltpu.make_async_copy(act.at[0, 0, :, :, pl.ds(col, CHUNK)], act_in.at[q], act_sem.at[q])

    grad_copy = pltpu.make_async_copy(grad, grad_in, act_sem.at[4])

    def w_fetch(src_w, src_s, block, q):
        rows = pl.ds(block * CHUNK, CHUNK)
        return (
            pltpu.make_async_copy(src_w.at[:, rows], w_buf.at[q], w_local.at[q, 0]),
            pltpu.make_async_copy(src_s.at[rows], s_buf.at[q], w_local.at[q, 1]),
        )

    @pl.when(stage == 0)
    def _():
        for q in range(N_CHUNKS):
            act_copy(q).start()

    @pl.when(stage == 1)
    def _():
        grad_copy.start()
        for q in range(2):
            for copy in w_fetch(w_own, s_own, q, q):
                copy.start()

    barrier = pltpu.get_barrier_semaphore()
    for target in ({"tp": 1 - t}, {"stage": 1 - stage}, {"dp": 1 - dp}):
        pl.semaphore_signal(barrier, inc=1, device_id=target, device_id_type=MESH)
    pl.semaphore_wait(barrier, 3)

    def remote(src, dst, sems, target):
        return pltpu.make_async_remote_copy(src_ref=src, dst_ref=dst, send_sem=sems.at[0], recv_sem=sems.at[1], device_id=target, device_id_type=MESH)

    peer, other_stage, other_dp = {"tp": 1 - t}, {"stage": 1 - stage}, {"dp": 1 - dp}

    def x_copy(q):
        return remote(xs.at[q], xr.at[q], x_sem.at[q], other_stage)

    def far_copy(q):
        return remote(xs.at[q], xr.at[q], far_sem.at[q], other_dp)

    def hop_copy(q):
        return remote(xr.at[q], x_far.at[q], hop_sem.at[q], other_stage)

    def dx_copy(q):
        return remote(xs.at[q], dx_in.at[q], dx_sem.at[q], other_stage)

    @pl.when(stage == 0)
    def _():
        pad[...] = jnp.zeros_like(pad)
        select = order_matrix(False)
        for q in range(N_CHUNKS):
            act_copy(q).wait()
            pad[:, :SIDE, :] = act_in[q]
            for lo in range(LO):
                rows = jnp.concatenate([pad[hi * LO + lo] for hi in range(4)], axis=0)
                xs[q, lo * 112:(lo + 1) * 112, :] = jnp.dot(select, rows, preferred_element_type=F32).astype(BF16)
            x_copy(q).start()
            far_copy(q).start()
        for q in range(N_CHUNKS):
            far_copy(q).wait_recv()
            hop_copy(q).start()
        for q in range(N_CHUNKS):
            x_copy(q).wait_send()
            far_copy(q).wait_send()
            hop_copy(q).wait_send()
            dx_copy(q).wait_recv()

    @pl.when(stage == 1)
    def _():
        w_copy = remote(w_own, w_peer, w_sem.at[0], peer)
        s_copy = remote(s_own, s_peer, w_sem.at[1], peer)
        vec_copies = [remote(ref, vec_peer.at[k], vec_sem.at[k], peer) for k, ref in enumerate((gam, bet, gms))]
        w_copy.start()
        s_copy.start()
        for copy in vec_copies:
            copy.start()

        grad_copy.wait()
        for image, dst in ((1 - t, dz_send), (t, dz_own)):
            select = pair_matrix(image, False)
            for lo in range(LO):
                rows = jnp.concatenate([grad_in[hi * LO + lo].reshape(56, HALF) for hi in range(4)], axis=0)
                dst[lo * 112:(lo + 1) * 112, :] = jnp.dot(select, rows, preferred_element_type=F32).astype(BF16)
        dz_copy = remote(dz_send, dz_peer, peer_sem.at[0], peer)
        dz_copy.start()

        def near_copy(q):
            return remote(xr.at[q], xn.at[q - 2], near_sem.at[q - 2], peer)

        def chunk(q, carry):
            x_copy(q).wait_recv()

            @pl.when(q >= 2)
            def _():
                near_copy(q).start()

            fill_halo(xh, xr[q])
            for i in range(3):
                for j in range(3):
                    k = i * 3 + j
                    im[:, k * CHUNK:(k + 1) * CHUNK] = window(xh, i, j)

            @pl.when(q == 1)
            def _():
                w_copy.wait_recv()
                s_copy.wait_recv()
                for k in range(2):
                    for copy in w_fetch(w_peer, s_peer, k, k + 2):
                        copy.start()

            for copy in w_fetch(w_own, s_own, 0, q):
                copy.wait()
            for n in range(2):
                cols = slice(n * HALF, (n + 1) * HALF)
                main = jnp.dot(im[...], w_buf[q, :, :, cols].reshape(9 * CHUNK, HALF), preferred_element_type=F32)
                side = jnp.dot(xr[q], s_buf[q, :, cols], preferred_element_type=F32)

                @pl.when(q == 0)
                def _():
                    pre[:, cols] = main
                    short[:, cols] = side

                @pl.when(q > 0)
                def _():
                    pre[:, cols] += main
                    short[:, cols] += side

            return carry

        lax.fori_loop(0, N_CHUNKS, chunk, 0)

        for copy in vec_copies:
            copy.wait_recv()
        dz_copy.wait_recv()
        for n in range(CH // TILE):
            half, part = n // 2, slice((n % 2) * TILE, (n % 2 + 1) * TILE)
            cols = slice(n * TILE, (n + 1) * TILE)
            mine = t == half
            gamma, beta, gamma_s = (jnp.where(mine, ref[:, part], vec_peer[k, :, part]) for k, ref in enumerate((gam, bet, gms)))
            for k, row in enumerate((gamma, beta, gamma_s)):
                vec_out[k:k + 1, cols] = row
            u = pre[:, cols] * gamma + beta + short[:, cols] * gamma_s
            z_st[:, cols] = jnp.maximum(u, 0.0).astype(BF16)
            dz = jnp.where(mine, dz_own[:, part].astype(F32), dz_peer[:, part].astype(F32))
            dz = jnp.where(u > 0.0, dz, 0.0)
            dzm_st[:, cols] = dz.astype(BF16)
            g_st[HAL * HAL:, :, cols] = (dz * gamma_s).astype(BF16).reshape(LO * LO, GRP, TILE)
            fill_halo(g_st.at[:, :, cols], (dz * gamma).astype(BF16))

        dzm_copy = remote(dzm_st, dzm_far, dzm_sem.at[0], other_dp)
        g_copy = remote(g_st, g_near, peer_sem.at[1], peer)
        mine_at, theirs_at = pl.multiple_of(t * HALF, HALF), pl.multiple_of((1 - t) * HALF, HALF)
        z_copy = remote(z_st.at[:, pl.ds(theirs_at, HALF)], z_near, peer_sem.at[2], peer)
        z_keep = pltpu.make_async_copy(z_st.at[:, pl.ds(mine_at, HALF)], z_out, keep_sem)
        for copy in (dzm_copy, g_copy, z_copy, z_keep):
            copy.start()

        def dx_chunk(q, carry):
            total = dot_nt(g_st[HAL * HAL:].reshape(PIX, CH), s_buf[q])
            for k in range(9):
                total = total + dot_nt(window(g_st, 2 - k // 3, 2 - k % 3), w_buf[q, k])
            xs[q] = total.astype(BF16)
            dx_copy(q).start()
            return carry

        lax.fori_loop(0, N_CHUNKS, dx_chunk, 0)

        near_copy(2).wait_recv()
        near_copy(3).wait_recv()
        g_copy.wait_recv()
        tails = []
        for k, (x_ref, g_ref) in enumerate(((xr, g_st), (xn, g_near))):
            tails.append(pltpu.make_async_copy(x_ref.at[0:2, MAIN:PIX], x_tails.at[k], tail_sem.at[k, 0]))
            for i in range(3):
                at = (LO - 1 + i) * HAL + LO - 1
                tails.append(pltpu.make_async_copy(g_ref.at[at:at + 3], g_tails.at[k, 3 * i:3 * i + 3], tail_sem.at[k, 1 + i]))
            tails.append(pltpu.make_async_copy(g_ref.at[GROUPS - 1:GROUPS], g_tails.at[k, 9:10], tail_sem.at[k, 4]))
        for copy in tails:
            copy.start()
        for q in range(2):
            rows = slice(q * CHUNK, (q + 1) * CHUNK)
            im[rows, :MAIN] = xr[q, :MAIN, :].T
            im[rows, MAIN:2 * MAIN] = xn[q, :MAIN, :].T

        def diag_copy(k):
            return remote(x_far.at[2 + k], x_diag.at[k], diag_sem.at[k], peer)

        dzm_diag_copy = remote(dzm_far, dzm_diag, dzm_sem.at[1], peer)

        def sum_copy(tap, k):
            return pltpu.make_async_copy((pre, short)[k].at[:HALF], sums.at[tap], sum_sem.at[k])

        def sum_pair(p, carry):
            @pl.when(p == 2)
            def _():
                for k in range(2):
                    hop_copy(2 + k).wait_recv()
                    diag_copy(k).start()

            @pl.when(p == 4)
            def _():
                dzm_copy.wait_recv()
                dzm_diag_copy.start()

            for k in range(2):
                tap = 2 * p + k
                rows = jnp.concatenate([tap_rows(g_st, tap), tap_rows(g_near, tap)], axis=0)
                total = jnp.dot(im[:HALF, :2 * MAIN], rows, preferred_element_type=F32)

                @pl.when(p > 0)
                def _():
                    sum_copy(tap - 2, k).wait()

                (pre, short)[k][:HALF] = total
                sum_copy(tap, k).start()
            return carry

        lax.fori_loop(0, 5, sum_pair, 0)

        for k in range(2):
            sum_copy(8 + k, k).wait()
            hop_copy(k).wait_recv()
            near_copy(2 + k).wait_send()
            diag_copy(k).wait()
        for q in range(N_CHUNKS):
            dx_copy(q).wait_send()
        for copy in tails:
            copy.wait()
        z_keep.wait()
        z_copy.wait()
        dzm_diag_copy.wait()
        for copy in [w_copy, s_copy, dz_copy, dzm_copy, g_copy] + vec_copies:
            copy.wait_send()


def main(act_in, grad_z, gamma, beta, gamma_s, w_own, s_own):
    vmem = pl.BlockSpec(memory_space=pltpu.VMEM)
    anywhere = pl.BlockSpec(memory_space=pl.ANY)
    dma = pltpu.SemaphoreType.DMA
    chunks = (N_CHUNKS, PIX, CHUNK)
    return pl.pallas_call(
        main_kernel,
        in_specs=[anywhere] * 2 + [vmem] * 3 + [anywhere] * 2,
        out_specs=[anywhere] * 5 + [vmem] + [anywhere] * 7,
        out_shape=[
            jax.ShapeDtypeStruct(chunks, BF16),
            jax.ShapeDtypeStruct((2, PIX, CHUNK), BF16),
            jax.ShapeDtypeStruct((2, 2, GRP, CHUNK), BF16),
            jax.ShapeDtypeStruct((9, HALF, CH), BF16),
            jax.ShapeDtypeStruct((HALF, CH), BF16),
            jax.ShapeDtypeStruct((3, CH), F32),
            jax.ShapeDtypeStruct((PIX, HALF), BF16),
            jax.ShapeDtypeStruct((PIX, HALF), BF16),
            jax.ShapeDtypeStruct((PIX, CH), BF16),
            jax.ShapeDtypeStruct((PIX, CH), BF16),
            jax.ShapeDtypeStruct((2, 10, GRP, CH), BF16),
            jax.ShapeDtypeStruct(chunks, BF16),
            jax.ShapeDtypeStruct((10, HALF, CH), F32),
        ],
        scratch_shapes=[
            pltpu.VMEM((N_CHUNKS, SIDE, SIDE, CHUNK), BF16),
            pltpu.VMEM((SIDE, 32, CHUNK), BF16),
            pltpu.VMEM(chunks, BF16),
            pltpu.VMEM(chunks, BF16),
            pltpu.VMEM((2, PIX, CHUNK), BF16),
            pltpu.VMEM((HAL * HAL, GRP, CHUNK), BF16),
            pltpu.VMEM((PIX, 9 * CHUNK), BF16),
            pltpu.VMEM((N_CHUNKS, 9, CHUNK, CH), BF16),
            pltpu.VMEM((N_CHUNKS, CHUNK, CH), BF16),
            pltpu.VMEM((PIX, CH), F32),
            pltpu.VMEM((PIX, CH), F32),
            pltpu.VMEM((SIDE, SIDE, 2, HALF), BF16),
            pltpu.VMEM((PIX, HALF), BF16),
            pltpu.VMEM((PIX, HALF), BF16),
            pltpu.VMEM((PIX, HALF), BF16),
            pltpu.VMEM((3, 1, HALF), F32),
            pltpu.VMEM((PIX, CH), BF16),
            pltpu.VMEM((PIX, CH), BF16),
            pltpu.VMEM((GROUPS, GRP, CH), BF16),
            pltpu.VMEM((GROUPS, GRP, CH), BF16),
            dma((5,)), dma((4, 2)), dma((4, 2)), dma((4, 2)), dma((2, 2)), dma((2, 2)), dma((2, 2)), dma((3, 2)), dma((3, 2)), dma((2, 2)),
            dma((4, 2)), dma((4, 2)), dma, dma((2, 5)), dma, dma((2,)),
        ],
        compiler_params=pltpu.CompilerParams(collective_id=0, has_side_effects=True, vmem_limit_bytes=66 * 1000 * 1000),
        cost_estimate=cost(6 * FWD_FLOPS, 2 * W_BYTES),
        name="main",
    )(act_in, jnp.transpose(grad_z[0], (1, 2, 0, 3)), gamma, beta, gamma_s, w_own, s_own)


def last_kernel(idx_ref, xa_ref, xb_ref, x_tails, dza_ref, dzb_ref, vec_ref, g_tails, dw_in, dw_ref, ds_ref, ga_ref, gb_ref, xt_ref):
    step = pl.program_id(0)
    stage = idx_ref[1]

    @pl.when((step == 0) & (stage == 1))
    def _():
        for q in range(2):
            rows = slice(q * CHUNK, (q + 1) * CHUNK)
            xt_ref[rows, :MAIN] = xa_ref[q, :MAIN, :].T
            xt_ref[rows, MAIN:2 * MAIN] = xb_ref[q, :MAIN, :].T
            ends = [xa_ref[q, MAIN:, :], xb_ref[q, MAIN:, :], x_tails[0, q], x_tails[1, q]]
            xt_ref[rows, 2 * MAIN:] = jnp.concatenate(ends, axis=0).T
        for dz_ref, g_ref in ((dza_ref, ga_ref), (dzb_ref, gb_ref)):
            for n in range(CH // TILE):
                cols = slice(n * TILE, (n + 1) * TILE)
                both_grads(dz_ref[:, cols].astype(F32), vec_ref.at[:, cols], g_ref.at[:, :, cols])

    @pl.when(stage == 0)
    def _():
        dw_ref[...] = jnp.zeros_like(dw_ref)
        ds_ref[...] = jnp.zeros_like(ds_ref)

    @pl.when(stage == 1)
    def _():
        last = step // 9
        i, j = 2 - step // 3, 2 - step % 3
        end = (1 - last) * (i * 3 + j) + last * 9
        final = (1 - last) * ((LO - 1 + i) * HAL + LO - 1 + j) + last * (GROUPS - 1)
        parts = [tap_rows(ga_ref, step), tap_rows(gb_ref, step), ga_ref[final], gb_ref[final], g_tails[0, end], g_tails[1, end]]
        total = jnp.dot(xt_ref[...], jnp.concatenate(parts, axis=0), preferred_element_type=F32) + dw_in[...]

        @pl.when(step < 9)
        def _():
            dw_ref[...] = total

        @pl.when(step == 9)
        def _():
            ds_ref[...] = total


def last_sums(idx, x_far, x_diag, x_tails, dzm_far, dzm_diag, vec, g_tails, sums):
    def whole(shape):
        return pl.BlockSpec(shape, lambda s, m: (0,) * len(shape))

    return pl.pallas_call(
        last_kernel,
        grid_spec=pltpu.PrefetchScalarGridSpec(
            num_scalar_prefetch=1,
            grid=(10,),
            in_specs=[
                whole((2, PIX, CHUNK)),
                whole((2, PIX, CHUNK)),
                whole((2, 2, GRP, CHUNK)),
                whole((PIX, CH)),
                whole((PIX, CH)),
                whole((3, CH)),
                whole((2, 10, GRP, CH)),
                pl.BlockSpec((None, HALF, CH), lambda s, m: (s, 0, 0)),
            ],
            out_specs=[
                pl.BlockSpec((None, None, None, HALF, CH), lambda s, m: (0, jnp.minimum(s, 8) // 3, jnp.minimum(s, 8) % 3, 0, 0)),
                pl.BlockSpec((None, HALF, CH), lambda s, m: (0, 0, 0)),
            ],
            scratch_shapes=[
                pltpu.VMEM((GROUPS, GRP, CH), BF16),
                pltpu.VMEM((GROUPS, GRP, CH), BF16),
                pltpu.VMEM((HALF, 2 * PIX + 2 * GRP), BF16),
            ],
        ),
        out_shape=[jax.ShapeDtypeStruct((1, 3, 3, HALF, CH), F32), jax.ShapeDtypeStruct((1, HALF, CH), F32)],
        compiler_params=params(1),
        cost_estimate=cost(2 * FWD_FLOPS, 2 * W_BYTES),
        name="last_sums",
    )(idx, x_far, x_diag, x_tails, dzm_far, dzm_diag, vec, g_tails, sums)


def solution(mesh):
    act_spec = P("stage", ("dp", "tp"), None, None, None)
    kernel_spec = P("stage", None, None, "tp", None)
    short_spec = P("stage", "tp", None)
    vec_spec = P("stage", "tp")
    grad_spec = P("stage", "dp", None, None, "tp")

    def device_step(act_in, w_conv, w_short, gamma, beta, gamma_s, grad_z):
        idx = jnp.stack([lax.axis_index("tp"), lax.axis_index("stage")]).astype(jnp.int32)
        w_own = w_conv.reshape(9, HALF, CH)
        s_own = w_short.reshape(HALF, CH)
        x_far, x_diag, x_tails, _, _, vec, z, z_near, dzm_far, dzm_diag, g_tails, dx, sums = main(act_in, grad_z, gamma, beta, gamma_s, w_own, s_own)
        z_out, grad_act = from_blocks(idx, z, z_near, dx)
        dw, ds = last_sums(idx, x_far, x_diag, x_tails, dzm_far, dzm_diag, vec, g_tails, sums)
        return z_out, grad_act, dw, ds

    return jax.shard_map(device_step, mesh=mesh, in_specs=(act_spec, kernel_spec, short_spec, vec_spec, vec_spec, vec_spec, grad_spec), out_specs=(grad_spec, act_spec, kernel_spec, short_spec), check_vma=False)
```

```python
import jax
import jax.numpy as jnp
from jax import lax
from jax.experimental import pallas as pl
from jax.experimental.pallas import tpu as pltpu
from jax.sharding import PartitionSpec as P

SIDE = 28
LO = 7
GRP = 16
HAL = LO + 2
GROUPS = HAL * HAL + LO * LO
PIX = SIDE * SIDE
HALF = 512
CH = 1024
TILE = 256
CHUNK = 256
N_CHUNKS = CH // CHUNK
MAIN = 768
MESH = pl.DeviceIdType.MESH
F32 = jnp.float32
BF16 = jnp.bfloat16
VMEM_LIMIT = 60 * 1024 * 1024


def params(n_axes):
    return pltpu.CompilerParams(dimension_semantics=("arbitrary",) * n_axes, vmem_limit_bytes=VMEM_LIMIT)


def cost(flops, bytes_accessed):
    return pl.CostEstimate(flops=int(flops), bytes_accessed=int(bytes_accessed), transcendentals=0)


def order_matrix(transposed):
    shape = (128, 112) if transposed else (112, 128)
    row = lax.broadcasted_iota(jnp.int32, shape, 1 if transposed else 0)
    col = lax.broadcasted_iota(jnp.int32, shape, 0 if transposed else 1)
    w_lo, h_hi, w_hi = row // 16, (row // 4) % 4, row % 4
    return (col == h_hi * 32 + w_hi * 7 + w_lo).astype(F32).astype(BF16)


def pair_matrix(first, transposed):
    shape = (224, 224) if transposed else (112, 224)
    row = lax.broadcasted_iota(jnp.int32, shape, 1 if transposed else 0)
    col = lax.broadcasted_iota(jnp.int32, shape, 0 if transposed else 1)
    image = (row // 112 + first) % 2
    row = row % 112
    w_lo, h_hi, w_hi = row // 16, (row // 4) % 4, row % 4
    return (col == h_hi * 56 + (w_hi * 7 + w_lo) * 2 + image).astype(F32).astype(BF16)


def moved(tile, step_h, step_w):
    wide = tile.astype(F32)
    n = wide.shape[1]
    if step_h < 0:
        wide = jnp.concatenate([jnp.zeros((4, n), F32), wide[:12]], axis=0)
    if step_h > 0:
        wide = jnp.concatenate([wide[4:], jnp.zeros((4, n), F32)], axis=0)
    if step_w:
        w_hi = lax.broadcasted_iota(jnp.int32, (GRP, n), 0) % 4
        if step_w < 0:
            wide = jnp.concatenate([wide[15:], wide[:15]], axis=0)
            wide = jnp.where(w_hi == 0, 0.0, wide)
        else:
            wide = jnp.concatenate([wide[1:], wide[:1]], axis=0)
            wide = jnp.where(w_hi == 3, 0.0, wide)
    return wide.astype(BF16)


def fill_halo(dst_ref, value):
    n = value.shape[1]
    groups = value.reshape(LO, LO, GRP, n)
    for a in range(HAL):
        step_h = -1 if a == 0 else (1 if a == HAL - 1 else 0)
        if not step_h:
            dst_ref[a * HAL + 1:a * HAL + 1 + LO] = groups[a - 1]
        for b in range(HAL):
            step_w = -1 if b == 0 else (1 if b == HAL - 1 else 0)
            if step_h or step_w:
                dst_ref[a * HAL + b] = moved(groups[(a - 1) % LO, (b - 1) % LO], step_h, step_w)


def window(ref, i, j):
    parts = [ref[pl.ds((i + a) * HAL + j, LO)] for a in range(LO)]
    whole = jnp.concatenate(parts, axis=0)
    return whole.reshape(PIX, whole.shape[-1])


FWD_FLOPS = 2 * PIX * HALF * CH * 10
W_BYTES = 10 * HALF * CH * 2


def dot_nt(a, b):
    return lax.dot_general(a, b, (((1,), (1,)), ((), ())), preferred_element_type=F32)


def tap_rows(ref, tap):
    last = tap // 9
    base = (1 - last) * ((2 - tap // 3) * HAL + 2 - tap % 3) + last * HAL * HAL
    pitch = HAL - 2 * last
    parts = [ref[pl.ds(base + a * pitch, LO if a < LO - 1 else LO - 1)] for a in range(LO)]
    return jnp.concatenate(parts, axis=0).reshape(MAIN, CH)


def main_kernel(
    act, grad, gam, bet, gms, w_own, s_own,
    x_far, x_diag, x_tails, w_peer, s_peer, vec_out, z_out, z_near, dzm_far, dzm_diag, g_tails, dx_in, sums,
    act_in, pad, xs, xr, xn, xh, im, w_buf, s_buf, pre, short, grad_in, dz_own, dz_send, dz_peer, vec_peer, z_st, dzm_st, g_st, g_near,
    act_sem, x_sem, far_sem, hop_sem, near_sem, diag_sem, w_sem, vec_sem, peer_sem, g_sem, dzm_sem, dx_sem, w_local, keep_sem, tail_sem, out_sem, sum_sem,
):
    t = lax.axis_index("tp")
    stage = lax.axis_index("stage")
    dp = lax.axis_index("dp")

    def act_copy(q):
        col = pl.multiple_of(lax.rem(t * HALF + q * CHUNK, CH), CHUNK)
        return pltpu.make_async_copy(act.at[0, 0, :, :, pl.ds(col, CHUNK)], act_in.at[q], act_sem.at[q])

    grad_copy = pltpu.make_async_copy(grad, grad_in, act_sem.at[4])

    def w_fetch(src_w, src_s, block, q):
        rows = pl.ds(block * CHUNK, CHUNK)
        return (
            pltpu.make_async_copy(src_w.at[:, rows], w_buf.at[q], w_local.at[q, 0]),
            pltpu.make_async_copy(src_s.at[rows], s_buf.at[q], w_local.at[q, 1]),
        )

    @pl.when(stage == 0)
    def _():
        for q in range(N_CHUNKS):
            act_copy(q).start()

    @pl.when(stage == 1)
    def _():
        grad_copy.start()
        for q in range(2):
            for copy in w_fetch(w_own, s_own, q, q):
                copy.start()

    barrier = pltpu.get_barrier_semaphore()
    for target in ({"tp": 1 - t}, {"stage": 1 - stage}, {"dp": 1 - dp}):
        pl.semaphore_signal(barrier, inc=1, device_id=target, device_id_type=MESH)
    pl.semaphore_wait(barrier, 3)

    def remote(src, dst, sems, target):
        return pltpu.make_async_remote_copy(src_ref=src, dst_ref=dst, send_sem=sems.at[0], recv_sem=sems.at[1], device_id=target, device_id_type=MESH)

    peer, other_stage, other_dp = {"tp": 1 - t}, {"stage": 1 - stage}, {"dp": 1 - dp}

    def x_copy(q):
        return remote(xs.at[q], xr.at[q], x_sem.at[q], other_stage)

    def far_copy(q):
        return remote(xs.at[q], xr.at[q], far_sem.at[q], other_dp)

    def hop_copy(q):
        return remote(xr.at[q], x_far.at[q], hop_sem.at[q], other_stage)

    def dx_copy(q):
        return remote(xs.at[q], dx_in.at[q], dx_sem.at[q], other_stage)

    @pl.when(stage == 0)
    def _():
        pad[...] = jnp.zeros_like(pad)
        select = order_matrix(False)
        for q in range(N_CHUNKS):
            act_copy(q).wait()
            pad[:, :SIDE, :] = act_in[q]
            for lo in range(LO):
                rows = jnp.concatenate([pad[hi * LO + lo] for hi in range(4)], axis=0)
                xs[q, lo * 112:(lo + 1) * 112, :] = jnp.dot(select, rows, preferred_element_type=F32).astype(BF16)
            x_copy(q).start()
            far_copy(q).start()
        for q in range(N_CHUNKS):
            far_copy(q).wait_recv()
            hop_copy(q).start()
        for q in range(N_CHUNKS):
            x_copy(q).wait_send()
            far_copy(q).wait_send()
            hop_copy(q).wait_send()
            dx_copy(q).wait_recv()

    @pl.when(stage == 1)
    def _():
        w_copy = remote(w_own, w_peer, w_sem.at[0], peer)
        s_copy = remote(s_own, s_peer, w_sem.at[1], peer)
        vec_copies = [remote(ref, vec_peer.at[k], vec_sem.at[k], peer) for k, ref in enumerate((gam, bet, gms))]
        w_copy.start()
        s_copy.start()
        for copy in vec_copies:
            copy.start()

        grad_copy.wait()
        for image, dst in ((1 - t, dz_send), (t, dz_own)):
            select = pair_matrix(image, False)
            for lo in range(LO):
                rows = jnp.concatenate([grad_in[hi * LO + lo].reshape(56, HALF) for hi in range(4)], axis=0)
                dst[lo * 112:(lo + 1) * 112, :] = jnp.dot(select, rows, preferred_element_type=F32).astype(BF16)
        dz_copy = remote(dz_send, dz_peer, peer_sem.at[0], peer)
        dz_copy.start()

        def near_copy(q):
            return remote(xr.at[q], xn.at[q - 2], near_sem.at[q - 2], peer)

        def land(q):
            x_copy(q).wait_recv()
            fill_halo(xh, xr[q])
            for i in range(3):
                for j in range(3):
                    k = i * 3 + j
                    im[:, k * CHUNK:(k + 1) * CHUNK] = window(xh, i, j)

        def terms(q, cols):
            main = jnp.dot(im[...], w_buf[q, :, :, cols].reshape(9 * CHUNK, HALF), preferred_element_type=F32)
            return main, jnp.dot(xr[q], s_buf[q, :, cols], preferred_element_type=F32)

        def chunk(q, carry):
            land(q)

            @pl.when(q == 1)
            def _():
                w_copy.wait_recv()
                s_copy.wait_recv()
                for k in range(2):
                    for copy in w_fetch(w_peer, s_peer, k, k + 2):
                        copy.start()

            @pl.when(q == 2)
            def _():
                near_copy(q).start()

            for copy in w_fetch(w_own, s_own, 0, q):
                copy.wait()
            for n in range(2):
                cols = slice(n * HALF, (n + 1) * HALF)
                main, side = terms(q, cols)

                @pl.when(q == 0)
                def _():
                    pre[:, cols] = main
                    short[:, cols] = side

                @pl.when(q > 0)
                def _():
                    pre[:, cols] += main
                    short[:, cols] += side

            return carry

        lax.fori_loop(0, N_CHUNKS - 1, chunk, 0)

        for copy in vec_copies:
            copy.wait_recv()
        dz_copy.wait_recv()

        def dzm_copy(n):
            cols = slice(n * HALF, (n + 1) * HALF)
            return remote(dzm_st.at[:, cols], dzm_far.at[:, cols], dzm_sem.at[n], other_dp)

        def g_copy(n):
            cols = slice(n * HALF, (n + 1) * HALF)
            return remote(g_st.at[:, :, cols], g_near.at[:, :, cols], g_sem.at[n], peer)

        land(N_CHUNKS - 1)
        near_copy(3).start()
        for copy in w_fetch(w_own, s_own, 0, 3):
            copy.wait()
        for half in range(2):
            mine = t == half
            main, side = terms(N_CHUNKS - 1, slice(half * HALF, (half + 1) * HALF))
            for n in range(2):
                part = slice(n * TILE, (n + 1) * TILE)
                cols = slice(half * HALF + n * TILE, half * HALF + (n + 1) * TILE)
                gamma, beta, gamma_s = (jnp.where(mine, ref[:, part], vec_peer[k, :, part]) for k, ref in enumerate((gam, bet, gms)))
                for k, row in enumerate((gamma, beta, gamma_s)):
                    vec_out[k:k + 1, cols] = row
                u = (pre[:, cols] + main[:, part]) * gamma + beta + (short[:, cols] + side[:, part]) * gamma_s
                z_st[:, cols] = jnp.maximum(u, 0.0).astype(BF16)
                dz = jnp.where(mine, dz_own[:, part].astype(F32), dz_peer[:, part].astype(F32))
                dz = jnp.where(u > 0.0, dz, 0.0)
                dzm_st[:, cols] = dz.astype(BF16)
                g_st[HAL * HAL:, :, cols] = (dz * gamma_s).astype(BF16).reshape(LO * LO, GRP, TILE)
                fill_halo(g_st.at[:, :, cols], (dz * gamma).astype(BF16))
            dzm_copy(half).start()
            g_copy(half).start()

        mine_at, theirs_at = pl.multiple_of(t * HALF, HALF), pl.multiple_of((1 - t) * HALF, HALF)
        z_copy = remote(z_st.at[:, pl.ds(theirs_at, HALF)], z_near, peer_sem.at[2], peer)
        z_keep = pltpu.make_async_copy(z_st.at[:, pl.ds(mine_at, HALF)], z_out, keep_sem)
        z_copy.start()
        z_keep.start()

        def dx_chunk(q, carry):
            total = dot_nt(g_st[HAL * HAL:].reshape(PIX, CH), s_buf[q])
            for k in range(9):
                total = total + dot_nt(window(g_st, 2 - k // 3, 2 - k % 3), w_buf[q, k])
            xs[q] = total.astype(BF16)
            dx_copy(q).start()
            return carry

        lax.fori_loop(0, N_CHUNKS, dx_chunk, 0)

        near_copy(2).wait_recv()
        near_copy(3).wait_recv()
        g_copy(0).wait_recv()
        g_copy(1).wait_recv()
        tails = []
        for k, (x_ref, g_ref) in enumerate(((xr, g_st), (xn, g_near))):
            tails.append(pltpu.make_async_copy(x_ref.at[0:2, MAIN:PIX], x_tails.at[k], tail_sem.at[k, 0]))
            for i in range(3):
                at = (LO - 1 + i) * HAL + LO - 1
                tails.append(pltpu.make_async_copy(g_ref.at[at:at + 3], g_tails.at[k, 3 * i:3 * i + 3], tail_sem.at[k, 1 + i]))
            tails.append(pltpu.make_async_copy(g_ref.at[GROUPS - 1:GROUPS], g_tails.at[k, 9:10], tail_sem.at[k, 4]))
        for copy in tails:
            copy.start()
        for q in range(2):
            rows = slice(q * CHUNK, (q + 1) * CHUNK)
            im[rows, :MAIN] = xr[q, :MAIN, :].T
            im[rows, MAIN:2 * MAIN] = xn[q, :MAIN, :].T

        def diag_copy(k):
            return remote(x_far.at[2 + k], x_diag.at[k], diag_sem.at[k], peer)

        dzm_diag_copy = remote(dzm_far, dzm_diag, dzm_sem.at[2], peer)

        def sum_copy(tap, k):
            return pltpu.make_async_copy((pre, short)[k].at[:HALF], sums.at[tap], sum_sem.at[k])

        def sum_pair(p, carry):
            @pl.when(p == 2)
            def _():
                for k in range(2):
                    hop_copy(2 + k).wait_recv()
                    diag_copy(k).start()

            @pl.when(p == 4)
            def _():
                dzm_copy(0).wait_recv()
                dzm_copy(1).wait_recv()
                dzm_diag_copy.start()

            for k in range(2):
                tap = 2 * p + k
                rows = jnp.concatenate([tap_rows(g_st, tap), tap_rows(g_near, tap)], axis=0)
                total = jnp.dot(im[:HALF, :2 * MAIN], rows, preferred_element_type=F32)

                @pl.when(p > 0)
                def _():
                    sum_copy(tap - 2, k).wait()

                (pre, short)[k][:HALF] = total
                sum_copy(tap, k).start()
            return carry

        lax.fori_loop(0, 5, sum_pair, 0)

        for k in range(2):
            sum_copy(8 + k, k).wait()
            hop_copy(k).wait_recv()
            near_copy(2 + k).wait_send()
            diag_copy(k).wait()
        for q in range(N_CHUNKS):
            dx_copy(q).wait_send()
        for copy in tails:
            copy.wait()
        z_keep.wait()
        z_copy.wait()
        dzm_diag_copy.wait()
        for copy in [w_copy, s_copy, dz_copy, dzm_copy(0), dzm_copy(1), g_copy(0), g_copy(1)] + vec_copies:
            copy.wait_send()


def main(act_in, grad_z, gamma, beta, gamma_s, w_own, s_own):
    vmem = pl.BlockSpec(memory_space=pltpu.VMEM)
    anywhere = pl.BlockSpec(memory_space=pl.ANY)
    dma = pltpu.SemaphoreType.DMA
    chunks = (N_CHUNKS, PIX, CHUNK)
    return pl.pallas_call(
        main_kernel,
        in_specs=[anywhere] * 2 + [vmem] * 3 + [anywhere] * 2,
        out_specs=[anywhere] * 5 + [vmem] + [anywhere] * 7,
        out_shape=[
            jax.ShapeDtypeStruct(chunks, BF16),
            jax.ShapeDtypeStruct((2, PIX, CHUNK), BF16),
            jax.ShapeDtypeStruct((2, 2, GRP, CHUNK), BF16),
            jax.ShapeDtypeStruct((9, HALF, CH), BF16),
            jax.ShapeDtypeStruct((HALF, CH), BF16),
            jax.ShapeDtypeStruct((3, CH), F32),
            jax.ShapeDtypeStruct((PIX, HALF), BF16),
            jax.ShapeDtypeStruct((PIX, HALF), BF16),
            jax.ShapeDtypeStruct((PIX, CH), BF16),
            jax.ShapeDtypeStruct((PIX, CH), BF16),
            jax.ShapeDtypeStruct((2, 10, GRP, CH), BF16),
            jax.ShapeDtypeStruct(chunks, BF16),
            jax.ShapeDtypeStruct((10, HALF, CH), F32),
        ],
        scratch_shapes=[
            pltpu.VMEM((N_CHUNKS, SIDE, SIDE, CHUNK), BF16),
            pltpu.VMEM((SIDE, 32, CHUNK), BF16),
            pltpu.VMEM(chunks, BF16),
            pltpu.VMEM(chunks, BF16),
            pltpu.VMEM((2, PIX, CHUNK), BF16),
            pltpu.VMEM((HAL * HAL, GRP, CHUNK), BF16),
            pltpu.VMEM((PIX, 9 * CHUNK), BF16),
            pltpu.VMEM((N_CHUNKS, 9, CHUNK, CH), BF16),
            pltpu.VMEM((N_CHUNKS, CHUNK, CH), BF16),
            pltpu.VMEM((PIX, CH), F32),
            pltpu.VMEM((PIX, CH), F32),
            pltpu.VMEM((SIDE, SIDE, 2, HALF), BF16),
            pltpu.VMEM((PIX, HALF), BF16),
            pltpu.VMEM((PIX, HALF), BF16),
            pltpu.VMEM((PIX, HALF), BF16),
            pltpu.VMEM((3, 1, HALF), F32),
            pltpu.VMEM((PIX, CH), BF16),
            pltpu.VMEM((PIX, CH), BF16),
            pltpu.VMEM((GROUPS, GRP, CH), BF16),
            pltpu.VMEM((GROUPS, GRP, CH), BF16),
            dma((5,)), dma((4, 2)), dma((4, 2)), dma((4, 2)), dma((2, 2)), dma((2, 2)), dma((2, 2)), dma((3, 2)), dma((3, 2)), dma((2, 2)), dma((3, 2)),
            dma((4, 2)), dma((4, 2)), dma, dma((2, 5)), dma, dma((2,)),
        ],
        compiler_params=pltpu.CompilerParams(collective_id=0, has_side_effects=True, vmem_limit_bytes=66 * 1000 * 1000),
        cost_estimate=cost(6 * FWD_FLOPS, 2 * W_BYTES),
        name="main",
    )(act_in, jnp.transpose(grad_z[0], (1, 2, 0, 3)), gamma, beta, gamma_s, w_own, s_own)


SLOTS = 4


def last_kernel(
    xa, xb, x_tails, dza, dzb, vec_ref, g_tails, sums, z, z_near, dx,
    dw_out, ds_out, z_out, dx_out,
    xa_v, xb_v, dza_v, dzb_v, sum_v, tot_v, z_v, zn_v, dx_v, z_st, dx_st, ga_ref, gb_ref, gsa_ref, gsb_ref, xt_ref, in_sem, sum_sem, tot_sem, side_sem, out_sem,
):
    step = pl.program_id(0)
    t = lax.axis_index("tp")
    stage = lax.axis_index("stage")
    fetches = [
        pltpu.make_async_copy(src, dst, in_sem.at[k])
        for k, (src, dst) in enumerate(((xa.at[0:2], xa_v), (dza, dza_v), (xb, xb_v), (dzb, dzb_v)))
    ]
    sides = [pltpu.make_async_copy(src, dst, side_sem.at[k]) for k, (src, dst) in enumerate(((z, z_v), (z_near, zn_v), (dx, dx_v)))]
    outs = [pltpu.make_async_copy(src, dst, out_sem.at[k]) for k, (src, dst) in enumerate(((z_st, z_out), (dx_st, dx_out)))]

    def sum_fetch(term):
        return pltpu.make_async_copy(sums.at[(term + 9) % 10], sum_v.at[term % SLOTS], sum_sem.at[term % SLOTS])

    def tot_copy(term):
        tap = term - 1
        return pltpu.make_async_copy(tot_v.at[term % SLOTS], dw_out.at[0, tap // 3, tap % 3], tot_sem.at[term % SLOTS])

    short_copy = pltpu.make_async_copy(tot_v.at[0], ds_out.at[0], tot_sem.at[0])

    def product(parts):
        return jnp.dot(xt_ref[...], jnp.concatenate(parts, axis=0), preferred_element_type=F32)

    def tap_product(tap):
        i, j = 2 - tap // 3, 2 - tap % 3
        final = (LO - 1 + i) * HAL + LO - 1 + j
        end = i * 3 + j
        return product([tap_rows(ga_ref, tap), tap_rows(gb_ref, tap), ga_ref[final], gb_ref[final], g_tails[0, end], g_tails[1, end]])

    @pl.when((step == 0) & (stage == 1))
    def _():
        for copy in fetches:
            copy.start()
        images = ((xa_v, dza_v, ga_ref, gsa_ref), (xb_v, dzb_v, gb_ref, gsb_ref))
        for k, (x_v, dz_v, g_ref, gs_ref) in enumerate(images):
            fetches[2 * k].wait()
            for q in range(2):
                rows = slice(q * CHUNK, (q + 1) * CHUNK)
                xt_ref[rows, k * MAIN:(k + 1) * MAIN] = x_v[q, :MAIN, :].T
            fetches[2 * k + 1].wait()
            if k == 0:
                sum_fetch(0).start()
                sum_fetch(1).start()
            gs_ref[...] = (dz_v[...].astype(F32) * vec_ref[2:3, :]).astype(BF16)
        sides[0].start()
        sides[1].start()
        sum_fetch(2).start()
        sum_fetch(3).start()
        for q in range(2):
            rows = slice(q * CHUNK, (q + 1) * CHUNK)
            ends = [xa_v[q, MAIN:, :], xb_v[q, MAIN:, :], x_tails[0, q], x_tails[1, q]]
            xt_ref[rows, 2 * MAIN:] = jnp.concatenate(ends, axis=0).T
        sum_fetch(0).wait()
        sum_fetch(1).wait()
        total = product([gsa_ref[:MAIN], gsb_ref[:MAIN], gsa_ref[MAIN:], gsb_ref[MAIN:], g_tails[0, 9], g_tails[1, 9]])
        for x_v, dz_v, g_ref, gs_ref in images:
            for n in range(CH // TILE):
                cols = slice(n * TILE, (n + 1) * TILE)
                fill_halo(g_ref.at[:, :, cols], (dz_v[:, cols].astype(F32) * vec_ref[0:1, cols]).astype(BF16))
        tot_v[0] = total + sum_v[0]
        short_copy.start()
        tot_v[1] = tap_product(0) + sum_v[1]
        tot_copy(1).start()

    def drain(term):
        @pl.when(term == 4)
        def _():
            short_copy.wait()

        @pl.when(term != 4)
        def _():
            tot_copy(term - SLOTS).wait()

    @pl.when((step > 0) & (stage == 1))
    def _():
        @pl.when(step < 4)
        def _():
            sum_fetch(2 * step + 2).start()
            sum_fetch(2 * step + 3).start()

        @pl.when(step > 1)
        def _():
            drain(2 * step)
            drain(2 * step + 1)

        sum_fetch(2 * step).wait()
        sum_fetch(2 * step + 1).wait()
        for k in range(2):
            term = 2 * step + k
            tot_v[term % SLOTS] = tap_product(term - 1) + sum_v[term % SLOTS]
        tot_copy(2 * step).start()
        tot_copy(2 * step + 1).start()

    @pl.when((step == 0) & (stage == 0))
    def _():
        sides[2].start()
        z_st[...] = jnp.zeros_like(z_st)
        outs[0].start()
        tot_v[0] = jnp.zeros_like(tot_v[0])
        short_copy.start()
        short_copy.wait()
        sides[2].wait()
        select = order_matrix(True)
        for lo in range(LO):
            for q in range(N_CHUNKS):
                to = pl.multiple_of(lax.rem(t * HALF + q * CHUNK, CH), CHUNK)
                rows = jnp.dot(select, dx_v[q, lo * 112:(lo + 1) * 112, :], preferred_element_type=F32).astype(BF16)
                for hi in range(4):
                    dx_st[0, 0, hi * LO + lo, :, pl.ds(to, CHUNK)] = rows[hi * 32:hi * 32 + SIDE, :]
        outs[1].start()

        def clear(tap, carry):
            copy = pltpu.make_async_copy(tot_v.at[0], dw_out.at[0, tap // 3, tap % 3], tot_sem.at[0])
            copy.start()
            copy.wait()
            return carry

        lax.fori_loop(0, 9, clear, 0)

    @pl.when((step == 1) & (stage == 1))
    def _():
        dx_st[...] = jnp.zeros_like(dx_st)
        outs[1].start()
        for copy in sides[:2]:
            copy.wait()
        select = pair_matrix(t, True)
        for lo in range(LO):
            part = slice(lo * 112, (lo + 1) * 112)
            both = jnp.concatenate([z_v[part, :], zn_v[part, :]], axis=0)
            rows = jnp.dot(select, both, preferred_element_type=F32)
            for hi in range(4):
                z_st[hi * LO + lo] = rows[hi * 56:(hi + 1) * 56].astype(BF16).reshape(SIDE, 2, HALF)
        outs[0].start()

    @pl.when(step == 4)
    def _():
        for copy in outs:
            copy.wait()

    @pl.when((step == 4) & (stage == 1))
    def _():
        for term in range(6, 10):
            tot_copy(term).wait()


def last(x_far, x_diag, x_tails, dzm_far, dzm_diag, vec, g_tails, sums, z, z_near, dx):
    def whole(shape):
        return pl.BlockSpec(shape, lambda s: (0,) * len(shape))

    anywhere = pl.BlockSpec(memory_space=pl.ANY)
    dma = pltpu.SemaphoreType.DMA
    z_shape, dx_shape = (SIDE, SIDE, 2, HALF), (1, 1, SIDE, SIDE, CH)
    dw, ds, z_out, dx_out = pl.pallas_call(
        last_kernel,
        grid=(5,),
        in_specs=[anywhere, anywhere, whole((2, 2, GRP, CHUNK)), anywhere, anywhere, whole((3, CH)), whole((2, 10, GRP, CH))] + [anywhere] * 4,
        out_specs=[anywhere] * 4,
        out_shape=[
            jax.ShapeDtypeStruct((1, 3, 3, HALF, CH), F32),
            jax.ShapeDtypeStruct((1, HALF, CH), F32),
            jax.ShapeDtypeStruct(z_shape, BF16),
            jax.ShapeDtypeStruct(dx_shape, BF16),
        ],
        scratch_shapes=[
            pltpu.VMEM((2, PIX, CHUNK), BF16),
            pltpu.VMEM((2, PIX, CHUNK), BF16),
            pltpu.VMEM((PIX, CH), BF16),
            pltpu.VMEM((PIX, CH), BF16),
            pltpu.VMEM((SLOTS, HALF, CH), F32),
            pltpu.VMEM((SLOTS, HALF, CH), F32),
            pltpu.VMEM((PIX, HALF), BF16),
            pltpu.VMEM((PIX, HALF), BF16),
            pltpu.VMEM((N_CHUNKS, PIX, CHUNK), BF16),
            pltpu.VMEM(z_shape, BF16),
            pltpu.VMEM(dx_shape, BF16),
            pltpu.VMEM((HAL * HAL, GRP, CH), BF16),
            pltpu.VMEM((HAL * HAL, GRP, CH), BF16),
            pltpu.VMEM((PIX, CH), BF16),
            pltpu.VMEM((PIX, CH), BF16),
            pltpu.VMEM((HALF, 2 * PIX + 2 * GRP), BF16),
            dma((4,)), dma((SLOTS,)), dma((SLOTS,)), dma((3,)), dma((2,)),
        ],
        compiler_params=params(1),
        cost_estimate=cost(2 * FWD_FLOPS, 2 * W_BYTES),
        name="last",
    )(x_far, x_diag, x_tails, dzm_far, dzm_diag, vec, g_tails, sums, z, z_near, dx)
    return jnp.transpose(z_out, (2, 0, 1, 3))[None], dx_out, dw, ds


def solution(mesh):
    act_spec = P("stage", ("dp", "tp"), None, None, None)
    kernel_spec = P("stage", None, None, "tp", None)
    short_spec = P("stage", "tp", None)
    vec_spec = P("stage", "tp")
    grad_spec = P("stage", "dp", None, None, "tp")

    def device_step(act_in, w_conv, w_short, gamma, beta, gamma_s, grad_z):
        w_own = w_conv.reshape(9, HALF, CH)
        s_own = w_short.reshape(HALF, CH)
        x_far, x_diag, x_tails, _, _, vec, z, z_near, dzm_far, dzm_diag, g_tails, dx, sums = main(act_in, grad_z, gamma, beta, gamma_s, w_own, s_own)
        return last(x_far, x_diag, x_tails, dzm_far, dzm_diag, vec, g_tails, sums, z, z_near, dx)

    return jax.shard_map(device_step, mesh=mesh, in_specs=(act_spec, kernel_spec, short_spec, vec_spec, vec_spec, vec_spec, grad_spec), out_specs=(grad_spec, act_spec, kernel_spec, short_spec), check_vma=False)
```

```python
import jax
import jax.numpy as jnp
from jax import lax
from jax.experimental import pallas as pl
from jax.experimental.pallas import tpu as pltpu
from jax.sharding import PartitionSpec as P

SIDE = 28
LO = 7
GRP = 16
HAL = LO + 2
GROUPS = HAL * HAL + LO * LO
PIX = SIDE * SIDE
HALF = 512
CH = 1024
TILE = 256
CHUNK = 256
PART = CHUNK // 2
N_CHUNKS = CH // CHUNK
MAIN = 768
MESH = pl.DeviceIdType.MESH
F32 = jnp.float32
BF16 = jnp.bfloat16
VMEM_LIMIT = 60 * 1024 * 1024


def params(n_axes):
    return pltpu.CompilerParams(dimension_semantics=("arbitrary",) * n_axes, vmem_limit_bytes=VMEM_LIMIT)


def cost(flops, bytes_accessed):
    return pl.CostEstimate(flops=int(flops), bytes_accessed=int(bytes_accessed), transcendentals=0)


def order_matrix(transposed):
    shape = (128, 112) if transposed else (112, 128)
    row = lax.broadcasted_iota(jnp.int32, shape, 1 if transposed else 0)
    col = lax.broadcasted_iota(jnp.int32, shape, 0 if transposed else 1)
    w_lo, h_hi, w_hi = row // 16, (row // 4) % 4, row % 4
    return (col == h_hi * 32 + w_hi * 7 + w_lo).astype(F32).astype(BF16)


def pair_matrix(first, transposed):
    shape = (224, 224) if transposed else (112, 224)
    row = lax.broadcasted_iota(jnp.int32, shape, 1 if transposed else 0)
    col = lax.broadcasted_iota(jnp.int32, shape, 0 if transposed else 1)
    image = (row // 112 + first) % 2
    row = row % 112
    w_lo, h_hi, w_hi = row // 16, (row // 4) % 4, row % 4
    return (col == h_hi * 56 + (w_hi * 7 + w_lo) * 2 + image).astype(F32).astype(BF16)


def moved(tile, step_h, step_w):
    wide = tile.astype(F32)
    n = wide.shape[1]
    if step_h < 0:
        wide = jnp.concatenate([jnp.zeros((4, n), F32), wide[:12]], axis=0)
    if step_h > 0:
        wide = jnp.concatenate([wide[4:], jnp.zeros((4, n), F32)], axis=0)
    if step_w:
        w_hi = lax.broadcasted_iota(jnp.int32, (GRP, n), 0) % 4
        if step_w < 0:
            wide = jnp.concatenate([wide[15:], wide[:15]], axis=0)
            wide = jnp.where(w_hi == 0, 0.0, wide)
        else:
            wide = jnp.concatenate([wide[1:], wide[:1]], axis=0)
            wide = jnp.where(w_hi == 3, 0.0, wide)
    return wide.astype(BF16)


def fill_halo(dst_ref, value):
    n = value.shape[1]
    groups = value.reshape(LO, LO, GRP, n)
    for a in range(HAL):
        step_h = -1 if a == 0 else (1 if a == HAL - 1 else 0)
        if not step_h:
            dst_ref[a * HAL + 1:a * HAL + 1 + LO] = groups[a - 1]
        for b in range(HAL):
            step_w = -1 if b == 0 else (1 if b == HAL - 1 else 0)
            if step_h or step_w:
                dst_ref[a * HAL + b] = moved(groups[(a - 1) % LO, (b - 1) % LO], step_h, step_w)


def window(ref, i, j):
    parts = [ref[pl.ds((i + a) * HAL + j, LO)] for a in range(LO)]
    whole = jnp.concatenate(parts, axis=0)
    return whole.reshape(PIX, whole.shape[-1])


FWD_FLOPS = 2 * PIX * HALF * CH * 10
W_BYTES = 10 * HALF * CH * 2


def dot_nt(a, b):
    return lax.dot_general(a, b, (((1,), (1,)), ((), ())), preferred_element_type=F32)


def tap_rows(ref, tap):
    last = tap // 9
    base = (1 - last) * ((2 - tap // 3) * HAL + 2 - tap % 3) + last * HAL * HAL
    pitch = HAL - 2 * last
    parts = [ref[pl.ds(base + a * pitch, LO if a < LO - 1 else LO - 1)] for a in range(LO)]
    return jnp.concatenate(parts, axis=0).reshape(MAIN, CH)


def main_kernel(
    act, grad, gam, bet, gms, w_own, s_own,
    x_far, x_diag, x_tails, w_peer, s_peer, vec_out, z_out, z_near, dzm_far, dzm_diag, g_tails, dx_in, sums,
    act_in, pad, xs, xr, xn, xh, im, w_buf, s_buf, pre, short, grad_in, dz_own, dz_send, dz_peer, vec_peer, z_st, dzm_st, g_st, g_near,
    act_sem, x_sem, far_sem, hop_sem, near_sem, diag_sem, w_sem, vec_sem, peer_sem, g_sem, dzm_sem, dx_sem, w_local, keep_sem, tail_sem, out_sem, sum_sem,
):
    t = lax.axis_index("tp")
    stage = lax.axis_index("stage")
    dp = lax.axis_index("dp")

    def act_copy(q):
        col = pl.multiple_of(lax.rem(t * HALF + q * CHUNK, CH), CHUNK)
        return pltpu.make_async_copy(act.at[0, 0, :, :, pl.ds(col, CHUNK)], act_in.at[q], act_sem.at[q])

    grad_copy = pltpu.make_async_copy(grad, grad_in, act_sem.at[4])

    def w_fetch(src_w, src_s, block, q):
        rows = pl.ds(block * CHUNK, CHUNK)
        return (
            pltpu.make_async_copy(src_w.at[:, rows], w_buf.at[q], w_local.at[q, 0]),
            pltpu.make_async_copy(src_s.at[rows], s_buf.at[q], w_local.at[q, 1]),
        )

    @pl.when(stage == 0)
    def _():
        for q in range(N_CHUNKS):
            act_copy(q).start()

    @pl.when(stage == 1)
    def _():
        grad_copy.start()
        for q in range(2):
            for copy in w_fetch(w_own, s_own, q, q):
                copy.start()

    barrier = pltpu.get_barrier_semaphore()
    for target in ({"tp": 1 - t}, {"stage": 1 - stage}, {"dp": 1 - dp}):
        pl.semaphore_signal(barrier, inc=1, device_id=target, device_id_type=MESH)

    def arrange(q):
        select = order_matrix(False)
        act_copy(q).wait()
        pad[:, :SIDE, :] = act_in[q]
        for lo in range(LO):
            rows = jnp.concatenate([pad[hi * LO + lo] for hi in range(4)], axis=0)
            xs[q, lo * 112:(lo + 1) * 112, :] = jnp.dot(select, rows, preferred_element_type=F32).astype(BF16)

    @pl.when(stage == 0)
    def _():
        pad[...] = jnp.zeros_like(pad)
        arrange(0)

    pl.semaphore_wait(barrier, 3)

    def remote(src, dst, sems, target):
        return pltpu.make_async_remote_copy(src_ref=src, dst_ref=dst, send_sem=sems.at[0], recv_sem=sems.at[1], device_id=target, device_id_type=MESH)

    peer, other_stage, other_dp = {"tp": 1 - t}, {"stage": 1 - stage}, {"dp": 1 - dp}

    def x_copy(q):
        return remote(xs.at[q], xr.at[q], x_sem.at[q], other_stage)

    def end_copy(k):
        cols = slice(k * PART, (k + 1) * PART)
        return remote(xs.at[N_CHUNKS - 1, :, cols], xr.at[N_CHUNKS - 1, :, cols], x_sem.at[N_CHUNKS - 1 + k], other_stage)

    def far_copy(q):
        return remote(xs.at[q], xr.at[q], far_sem.at[q], other_dp)

    def hop_copy(q):
        return remote(xr.at[q], x_far.at[q], hop_sem.at[q], other_stage)

    def dx_copy(q):
        return remote(xs.at[q], dx_in.at[q], dx_sem.at[q], other_stage)

    @pl.when(stage == 0)
    def _():
        for q in range(N_CHUNKS):
            if q:
                arrange(q)
            if q < N_CHUNKS - 1:
                x_copy(q).start()
            else:
                end_copy(0).start()
                end_copy(1).start()
            far_copy(q).start()
        for q in range(N_CHUNKS):
            far_copy(q).wait_recv()
            hop_copy(q).start()
        for k in range(2):
            end_copy(k).wait_send()
        for q in range(N_CHUNKS):
            if q < N_CHUNKS - 1:
                x_copy(q).wait_send()
            far_copy(q).wait_send()
            hop_copy(q).wait_send()
        for q in range(N_CHUNKS):
            dx_copy(q).wait_recv()

    @pl.when(stage == 1)
    def _():
        w_copy = remote(w_own, w_peer, w_sem.at[0], peer)
        s_copy = remote(s_own, s_peer, w_sem.at[1], peer)
        vec_copies = [remote(ref, vec_peer.at[k], vec_sem.at[k], peer) for k, ref in enumerate((gam, bet, gms))]
        w_copy.start()
        s_copy.start()
        for copy in vec_copies:
            copy.start()

        grad_copy.wait()
        for image, dst in ((1 - t, dz_send), (t, dz_own)):
            select = pair_matrix(image, False)
            for lo in range(LO):
                rows = jnp.concatenate([grad_in[hi * LO + lo].reshape(56, HALF) for hi in range(4)], axis=0)
                dst[lo * 112:(lo + 1) * 112, :] = jnp.dot(select, rows, preferred_element_type=F32).astype(BF16)
        dz_copy = remote(dz_send, dz_peer, peer_sem.at[0], peer)
        dz_copy.start()

        def near_copy(q):
            return remote(xr.at[q], xn.at[q - 2], near_sem.at[q - 2], peer)

        def land(q, cols):
            n = cols.stop - cols.start
            halo = xh.at[:, :, :n]
            fill_halo(halo, xr[q, :, cols])
            for i in range(3):
                for j in range(3):
                    k = i * 3 + j
                    im[:, k * n:(k + 1) * n] = window(halo, i, j)

        def terms(q, rows, cols):
            k = 9 * (rows.stop - rows.start)
            main = jnp.dot(im[:, :k], w_buf[q, :, rows, cols].reshape(k, HALF), preferred_element_type=F32)
            return main, jnp.dot(xr[q, :, rows], s_buf[q, rows, cols], preferred_element_type=F32)

        whole = slice(0, CHUNK)

        def chunk(q, carry):
            x_copy(q).wait_recv()
            land(q, whole)

            @pl.when(q == 1)
            def _():
                w_copy.wait_recv()
                s_copy.wait_recv()
                for k in range(2):
                    for copy in w_fetch(w_peer, s_peer, k, k + 2):
                        copy.start()

            @pl.when(q == 2)
            def _():
                near_copy(q).start()

            for copy in w_fetch(w_own, s_own, 0, q):
                copy.wait()
            for n in range(2):
                cols = slice(n * HALF, (n + 1) * HALF)
                main, side = terms(q, whole, cols)

                @pl.when(q == 0)
                def _():
                    pre[:, cols] = main
                    short[:, cols] = side

                @pl.when(q > 0)
                def _():
                    pre[:, cols] += main
                    short[:, cols] += side

            return carry

        lax.fori_loop(0, N_CHUNKS - 1, chunk, 0)

        for copy in vec_copies:
            copy.wait_recv()
        dz_copy.wait_recv()

        def dzm_copy(n):
            cols = slice(n * HALF, (n + 1) * HALF)
            return remote(dzm_st.at[:, cols], dzm_far.at[:, cols], dzm_sem.at[n], other_dp)

        def g_copy(n):
            cols = slice(n * HALF, (n + 1) * HALF)
            return remote(g_st.at[:, :, cols], g_near.at[:, :, cols], g_sem.at[n], peer)

        for copy in w_fetch(w_own, s_own, 0, 3):
            copy.wait()
        end_copy(0).wait_recv()
        land(N_CHUNKS - 1, slice(0, PART))
        for n in range(2):
            cols = slice(n * HALF, (n + 1) * HALF)
            main, side = terms(N_CHUNKS - 1, slice(0, PART), cols)
            pre[:, cols] += main
            short[:, cols] += side
        end_copy(1).wait_recv()
        land(N_CHUNKS - 1, slice(PART, CHUNK))
        near_copy(3).start()
        for half in range(2):
            mine = t == half
            main, side = terms(N_CHUNKS - 1, slice(PART, CHUNK), slice(half * HALF, (half + 1) * HALF))
            for n in range(2):
                part = slice(n * TILE, (n + 1) * TILE)
                cols = slice(half * HALF + n * TILE, half * HALF + (n + 1) * TILE)
                gamma, beta, gamma_s = (jnp.where(mine, ref[:, part], vec_peer[k, :, part]) for k, ref in enumerate((gam, bet, gms)))
                for k, row in enumerate((gamma, beta, gamma_s)):
                    vec_out[k:k + 1, cols] = row
                u = (pre[:, cols] + main[:, part]) * gamma + beta + (short[:, cols] + side[:, part]) * gamma_s
                z_st[:, cols] = jnp.maximum(u, 0.0).astype(BF16)
                dz = jnp.where(mine, dz_own[:, part].astype(F32), dz_peer[:, part].astype(F32))
                dz = jnp.where(u > 0.0, dz, 0.0)
                dzm_st[:, cols] = dz.astype(BF16)
                g_st[HAL * HAL:, :, cols] = (dz * gamma_s).astype(BF16).reshape(LO * LO, GRP, TILE)
                fill_halo(g_st.at[:, :, cols], (dz * gamma).astype(BF16))
            dzm_copy(half).start()
            g_copy(half).start()

        mine_at, theirs_at = pl.multiple_of(t * HALF, HALF), pl.multiple_of((1 - t) * HALF, HALF)
        z_copy = remote(z_st.at[:, pl.ds(theirs_at, HALF)], z_near, peer_sem.at[2], peer)
        z_keep = pltpu.make_async_copy(z_st.at[:, pl.ds(mine_at, HALF)], z_out, keep_sem)
        z_copy.start()
        z_keep.start()

        def dx_chunk(q, carry):
            total = dot_nt(g_st[HAL * HAL:].reshape(PIX, CH), s_buf[q])
            for k in range(9):
                total = total + dot_nt(window(g_st, 2 - k // 3, 2 - k % 3), w_buf[q, k])
            xs[q] = total.astype(BF16)
            dx_copy(q).start()
            return carry

        lax.fori_loop(0, N_CHUNKS, dx_chunk, 0)

        near_copy(2).wait_recv()
        near_copy(3).wait_recv()
        g_copy(0).wait_recv()
        g_copy(1).wait_recv()
        tails = []
        for k, (x_ref, g_ref) in enumerate(((xr, g_st), (xn, g_near))):
            tails.append(pltpu.make_async_copy(x_ref.at[0:2, MAIN:PIX], x_tails.at[k], tail_sem.at[k, 0]))
            for i in range(3):
                at = (LO - 1 + i) * HAL + LO - 1
                tails.append(pltpu.make_async_copy(g_ref.at[at:at + 3], g_tails.at[k, 3 * i:3 * i + 3], tail_sem.at[k, 1 + i]))
            tails.append(pltpu.make_async_copy(g_ref.at[GROUPS - 1:GROUPS], g_tails.at[k, 9:10], tail_sem.at[k, 4]))
        for copy in tails:
            copy.start()
        for q in range(2):
            rows = slice(q * CHUNK, (q + 1) * CHUNK)
            im[rows, :MAIN] = xr[q, :MAIN, :].T
            im[rows, MAIN:2 * MAIN] = xn[q, :MAIN, :].T

        def diag_copy(k):
            return remote(x_far.at[2 + k], x_diag.at[k], diag_sem.at[k], peer)

        def dzm_diag_copy(n):
            cols = slice(n * HALF, (n + 1) * HALF)
            return remote(dzm_far.at[:, cols], dzm_diag.at[:, cols], dzm_sem.at[2 + n], peer)

        def sum_copy(tap, k):
            return pltpu.make_async_copy((pre, short)[k].at[:HALF], sums.at[tap], sum_sem.at[k])

        def sum_pair(p, carry):
            @pl.when(p == 4)
            def _():
                for k in range(2):
                    hop_copy(2 + k).wait_recv()
                    diag_copy(k).start()

            for n in range(2):
                @pl.when(p == 3 + n)
                def _():
                    dzm_copy(n).wait_recv()
                    dzm_diag_copy(n).start()

            for k in range(2):
                tap = 2 * p + k
                rows = jnp.concatenate([tap_rows(g_st, tap), tap_rows(g_near, tap)], axis=0)
                total = jnp.dot(im[:HALF, :2 * MAIN], rows, preferred_element_type=F32)

                @pl.when(p > 0)
                def _():
                    sum_copy(tap - 2, k).wait()

                (pre, short)[k][:HALF] = total
                sum_copy(tap, k).start()
            return carry

        lax.fori_loop(0, 5, sum_pair, 0)

        for k in range(2):
            sum_copy(8 + k, k).wait()
            hop_copy(k).wait_recv()
            near_copy(2 + k).wait_send()
            diag_copy(k).wait()
        for q in range(N_CHUNKS):
            dx_copy(q).wait_send()
        for copy in tails:
            copy.wait()
        z_keep.wait()
        z_copy.wait()
        for n in range(2):
            dzm_diag_copy(n).wait()
        for copy in [w_copy, s_copy, dz_copy, dzm_copy(0), dzm_copy(1), g_copy(0), g_copy(1)] + vec_copies:
            copy.wait_send()


def main(act_in, grad_z, gamma, beta, gamma_s, w_own, s_own):
    vmem = pl.BlockSpec(memory_space=pltpu.VMEM)
    anywhere = pl.BlockSpec(memory_space=pl.ANY)
    dma = pltpu.SemaphoreType.DMA
    chunks = (N_CHUNKS, PIX, CHUNK)
    return pl.pallas_call(
        main_kernel,
        in_specs=[anywhere] * 2 + [vmem] * 3 + [anywhere] * 2,
        out_specs=[anywhere] * 5 + [vmem] + [anywhere] * 7,
        out_shape=[
            jax.ShapeDtypeStruct(chunks, BF16),
            jax.ShapeDtypeStruct((2, PIX, CHUNK), BF16),
            jax.ShapeDtypeStruct((2, 2, GRP, CHUNK), BF16),
            jax.ShapeDtypeStruct((9, HALF, CH), BF16),
            jax.ShapeDtypeStruct((HALF, CH), BF16),
            jax.ShapeDtypeStruct((3, CH), F32),
            jax.ShapeDtypeStruct((PIX, HALF), BF16),
            jax.ShapeDtypeStruct((PIX, HALF), BF16),
            jax.ShapeDtypeStruct((PIX, CH), BF16),
            jax.ShapeDtypeStruct((PIX, CH), BF16),
            jax.ShapeDtypeStruct((2, 10, GRP, CH), BF16),
            jax.ShapeDtypeStruct(chunks, BF16),
            jax.ShapeDtypeStruct((10, HALF, CH), F32),
        ],
        scratch_shapes=[
            pltpu.VMEM((N_CHUNKS, SIDE, SIDE, CHUNK), BF16),
            pltpu.VMEM((SIDE, 32, CHUNK), BF16),
            pltpu.VMEM(chunks, BF16),
            pltpu.VMEM(chunks, BF16),
            pltpu.VMEM((2, PIX, CHUNK), BF16),
            pltpu.VMEM((HAL * HAL, GRP, CHUNK), BF16),
            pltpu.VMEM((PIX, 9 * CHUNK), BF16),
            pltpu.VMEM((N_CHUNKS, 9, CHUNK, CH), BF16),
            pltpu.VMEM((N_CHUNKS, CHUNK, CH), BF16),
            pltpu.VMEM((PIX, CH), F32),
            pltpu.VMEM((PIX, CH), F32),
            pltpu.VMEM((SIDE, SIDE, 2, HALF), BF16),
            pltpu.VMEM((PIX, HALF), BF16),
            pltpu.VMEM((PIX, HALF), BF16),
            pltpu.VMEM((PIX, HALF), BF16),
            pltpu.VMEM((3, 1, HALF), F32),
            pltpu.VMEM((PIX, CH), BF16),
            pltpu.VMEM((PIX, CH), BF16),
            pltpu.VMEM((GROUPS, GRP, CH), BF16),
            pltpu.VMEM((GROUPS, GRP, CH), BF16),
            dma((5,)), dma((5, 2)), dma((4, 2)), dma((4, 2)), dma((2, 2)), dma((2, 2)), dma((2, 2)), dma((3, 2)), dma((3, 2)), dma((2, 2)), dma((4, 2)),
            dma((4, 2)), dma((4, 2)), dma, dma((2, 5)), dma, dma((2,)),
        ],
        compiler_params=pltpu.CompilerParams(collective_id=0, has_side_effects=True, vmem_limit_bytes=66 * 1000 * 1000),
        cost_estimate=cost(6 * FWD_FLOPS, 2 * W_BYTES),
        name="main",
    )(act_in, jnp.transpose(grad_z[0], (1, 2, 0, 3)), gamma, beta, gamma_s, w_own, s_own)


SLOTS = 4


def last_kernel(
    xa, xb, x_ends, dza, dzb, vec, g_ends, sums, z, z_near, dx,
    dw_out, ds_out, z_out, dx_out,
    xa_v, xb_v, dza_v, dzb_v, x_tails, vec_ref, g_tails, sum_v, tot_v, z_v, zn_v, dx_v, z_st, dx_st, ga_ref, gb_ref, gsa_ref, gsb_ref, xt_ref, in_sem, small_sem, sum_sem, tot_sem, side_sem, out_sem,
):
    step = pl.program_id(0)
    t = lax.axis_index("tp")
    stage = lax.axis_index("stage")
    fetches = [
        pltpu.make_async_copy(src, dst, in_sem.at[k])
        for k, (src, dst) in enumerate(((xa.at[0:2], xa_v), (dza, dza_v), (xb, xb_v), (dzb, dzb_v)))
    ]
    smalls = [pltpu.make_async_copy(src, dst, small_sem.at[k]) for k, (src, dst) in enumerate(((vec, vec_ref), (x_ends, x_tails), (g_ends, g_tails)))]
    sides = [pltpu.make_async_copy(src, dst, side_sem.at[k]) for k, (src, dst) in enumerate(((z, z_v), (z_near, zn_v), (dx, dx_v)))]
    outs = [pltpu.make_async_copy(src, dst, out_sem.at[k]) for k, (src, dst) in enumerate(((z_st, z_out), (dx_st, dx_out)))]

    def sum_fetch(term):
        return pltpu.make_async_copy(sums.at[(term + 9) % 10], sum_v.at[term % SLOTS], sum_sem.at[term % SLOTS])

    def tot_copy(term):
        tap = term - 1
        return pltpu.make_async_copy(tot_v.at[term % SLOTS], dw_out.at[0, tap // 3, tap % 3], tot_sem.at[term % SLOTS])

    short_copy = pltpu.make_async_copy(tot_v.at[0], ds_out.at[0], tot_sem.at[0])

    def product(parts):
        return jnp.dot(xt_ref[...], jnp.concatenate(parts, axis=0), preferred_element_type=F32)

    def tap_product(tap):
        i, j = 2 - tap // 3, 2 - tap % 3
        final = (LO - 1 + i) * HAL + LO - 1 + j
        end = i * 3 + j
        return product([tap_rows(ga_ref, tap), tap_rows(gb_ref, tap), ga_ref[final], gb_ref[final], g_tails[0, end], g_tails[1, end]])

    @pl.when((step == 0) & (stage == 1))
    def _():
        images = ((xa_v, dza_v, ga_ref, gsa_ref), (xb_v, dzb_v, gb_ref, gsb_ref))
        for copy in [smalls[0]] + fetches[:2] + smalls[1:]:
            copy.start()
        smalls[0].wait()
        for k, (x_v, dz_v, g_ref, gs_ref) in enumerate(images):
            fetches[2 * k].wait()
            for q in range(2):
                rows = slice(q * CHUNK, (q + 1) * CHUNK)
                xt_ref[rows, k * MAIN:(k + 1) * MAIN] = x_v[q, :MAIN, :].T
            fetches[2 * k + 1].wait()
            if k == 0:
                for copy in fetches[2:]:
                    copy.start()
            else:
                sum_fetch(0).start()
                sum_fetch(1).start()
            gs_ref[...] = (dz_v[...].astype(F32) * vec_ref[2:3, :]).astype(BF16)
            if k == 0:
                tot_v[0] = jnp.dot(xt_ref[:, :MAIN], gsa_ref[:MAIN], preferred_element_type=F32)
        for copy in smalls[1:]:
            copy.wait()
        for q in range(2):
            rows = slice(q * CHUNK, (q + 1) * CHUNK)
            ends = [xa_v[q, MAIN:, :], xb_v[q, MAIN:, :], x_tails[0, q], x_tails[1, q]]
            xt_ref[rows, 2 * MAIN:] = jnp.concatenate(ends, axis=0).T
        rest = jnp.concatenate([gsb_ref[:MAIN], gsa_ref[MAIN:], gsb_ref[MAIN:], g_tails[0, 9], g_tails[1, 9]], axis=0)
        total = jnp.dot(xt_ref[:, MAIN:], rest, preferred_element_type=F32)
        for x_v, dz_v, g_ref, gs_ref in images:
            for n in range(CH // TILE):
                cols = slice(n * TILE, (n + 1) * TILE)
                fill_halo(g_ref.at[:, :, cols], (dz_v[:, cols].astype(F32) * vec_ref[0:1, cols]).astype(BF16))
        for copy in sides[:2]:
            copy.start()
        sum_fetch(2).start()
        sum_fetch(3).start()
        sum_fetch(0).wait()
        tot_v[0] += total + sum_v[0]
        short_copy.start()
        sum_fetch(1).wait()
        tot_v[1] = tap_product(0) + sum_v[1]
        tot_copy(1).start()

    def drain(term):
        @pl.when(term == 4)
        def _():
            short_copy.wait()

        @pl.when(term != 4)
        def _():
            tot_copy(term - SLOTS).wait()

    @pl.when((step > 0) & (stage == 1))
    def _():
        @pl.when(step < 4)
        def _():
            sum_fetch(2 * step + 2).start()
            sum_fetch(2 * step + 3).start()

        @pl.when(step > 1)
        def _():
            drain(2 * step)
            drain(2 * step + 1)

        sum_fetch(2 * step).wait()
        sum_fetch(2 * step + 1).wait()
        for k in range(2):
            term = 2 * step + k
            tot_v[term % SLOTS] = tap_product(term - 1) + sum_v[term % SLOTS]
            tot_copy(term).start()

    @pl.when((step == 0) & (stage == 0))
    def _():
        sides[2].start()
        z_st[...] = jnp.zeros_like(z_st)
        outs[0].start()
        tot_v[0] = jnp.zeros_like(tot_v[0])
        short_copy.start()
        short_copy.wait()
        sides[2].wait()
        select = order_matrix(True)
        for lo in range(LO):
            for q in range(N_CHUNKS):
                to = pl.multiple_of(lax.rem(t * HALF + q * CHUNK, CH), CHUNK)
                rows = jnp.dot(select, dx_v[q, lo * 112:(lo + 1) * 112, :], preferred_element_type=F32).astype(BF16)
                for hi in range(4):
                    dx_st[0, 0, hi * LO + lo, :, pl.ds(to, CHUNK)] = rows[hi * 32:hi * 32 + SIDE, :]
        outs[1].start()

        def clear(tap, carry):
            copy = pltpu.make_async_copy(tot_v.at[0], dw_out.at[0, tap // 3, tap % 3], tot_sem.at[0])
            copy.start()
            copy.wait()
            return carry

        lax.fori_loop(0, 9, clear, 0)

    @pl.when((step == 1) & (stage == 1))
    def _():
        dx_st[...] = jnp.zeros_like(dx_st)
        outs[1].start()
        for copy in sides[:2]:
            copy.wait()
        select = pair_matrix(t, True)
        for lo in range(LO):
            part = slice(lo * 112, (lo + 1) * 112)
            both = jnp.concatenate([z_v[part, :], zn_v[part, :]], axis=0)
            rows = jnp.dot(select, both, preferred_element_type=F32)
            for hi in range(4):
                z_st[hi * LO + lo] = rows[hi * 56:(hi + 1) * 56].astype(BF16).reshape(SIDE, 2, HALF)
        outs[0].start()

    @pl.when(step == 4)
    def _():
        for copy in outs:
            copy.wait()

    @pl.when((step == 4) & (stage == 1))
    def _():
        for term in range(6, 10):
            tot_copy(term).wait()


def last(x_far, x_diag, x_tails, dzm_far, dzm_diag, vec, g_tails, sums, z, z_near, dx):
    anywhere = pl.BlockSpec(memory_space=pl.ANY)
    dma = pltpu.SemaphoreType.DMA
    z_shape, dx_shape = (SIDE, SIDE, 2, HALF), (1, 1, SIDE, SIDE, CH)
    dw, ds, z_out, dx_out = pl.pallas_call(
        last_kernel,
        grid=(5,),
        in_specs=[anywhere] * 11,
        out_specs=[anywhere] * 4,
        out_shape=[
            jax.ShapeDtypeStruct((1, 3, 3, HALF, CH), F32),
            jax.ShapeDtypeStruct((1, HALF, CH), F32),
            jax.ShapeDtypeStruct(z_shape, BF16),
            jax.ShapeDtypeStruct(dx_shape, BF16),
        ],
        scratch_shapes=[
            pltpu.VMEM((2, PIX, CHUNK), BF16),
            pltpu.VMEM((2, PIX, CHUNK), BF16),
            pltpu.VMEM((PIX, CH), BF16),
            pltpu.VMEM((PIX, CH), BF16),
            pltpu.VMEM((2, 2, GRP, CHUNK), BF16),
            pltpu.VMEM((3, CH), F32),
            pltpu.VMEM((2, 10, GRP, CH), BF16),
            pltpu.VMEM((SLOTS, HALF, CH), F32),
            pltpu.VMEM((SLOTS, HALF, CH), F32),
            pltpu.VMEM((PIX, HALF), BF16),
            pltpu.VMEM((PIX, HALF), BF16),
            pltpu.VMEM((N_CHUNKS, PIX, CHUNK), BF16),
            pltpu.VMEM(z_shape, BF16),
            pltpu.VMEM(dx_shape, BF16),
            pltpu.VMEM((HAL * HAL, GRP, CH), BF16),
            pltpu.VMEM((HAL * HAL, GRP, CH), BF16),
            pltpu.VMEM((PIX, CH), BF16),
            pltpu.VMEM((PIX, CH), BF16),
            pltpu.VMEM((HALF, 2 * PIX + 2 * GRP), BF16),
            dma((4,)), dma((3,)), dma((SLOTS,)), dma((SLOTS,)), dma((3,)), dma((2,)),
        ],
        compiler_params=params(1),
        cost_estimate=cost(2 * FWD_FLOPS, 2 * W_BYTES),
        name="last",
    )(x_far, x_diag, x_tails, dzm_far, dzm_diag, vec, g_tails, sums, z, z_near, dx)
    return jnp.transpose(z_out, (2, 0, 1, 3))[None], dx_out, dw, ds


def solution(mesh):
    act_spec = P("stage", ("dp", "tp"), None, None, None)
    kernel_spec = P("stage", None, None, "tp", None)
    short_spec = P("stage", "tp", None)
    vec_spec = P("stage", "tp")
    grad_spec = P("stage", "dp", None, None, "tp")

    def device_step(act_in, w_conv, w_short, gamma, beta, gamma_s, grad_z):
        w_own = w_conv.reshape(9, HALF, CH)
        s_own = w_short.reshape(HALF, CH)
        x_far, x_diag, x_tails, _, _, vec, z, z_near, dzm_far, dzm_diag, g_tails, dx, sums = main(act_in, grad_z, gamma, beta, gamma_s, w_own, s_own)
        return last(x_far, x_diag, x_tails, dzm_far, dzm_diag, vec, g_tails, sums, z, z_near, dx)

    return jax.shard_map(device_step, mesh=mesh, in_specs=(act_spec, kernel_spec, short_spec, vec_spec, vec_spec, vec_spec, grad_spec), out_specs=(grad_spec, act_spec, kernel_spec, short_spec), check_vma=False)
```

```python
import jax
import jax.numpy as jnp
from jax import lax
from jax.experimental import pallas as pl
from jax.experimental.pallas import tpu as pltpu
from jax.sharding import PartitionSpec as P

SIDE = 28
LO = 7
GRP = 16
HAL = LO + 2
GROUPS = HAL * HAL + LO * LO
PIX = SIDE * SIDE
HALF = 512
CH = 1024
TILE = 256
CHUNK = 256
PART = CHUNK // 2
N_CHUNKS = CH // CHUNK
MAIN = 768
MESH = pl.DeviceIdType.MESH
F32 = jnp.float32
BF16 = jnp.bfloat16
VMEM_LIMIT = 60 * 1024 * 1024


def params(n_axes):
    return pltpu.CompilerParams(dimension_semantics=("arbitrary",) * n_axes, vmem_limit_bytes=VMEM_LIMIT)


def cost(flops, bytes_accessed):
    return pl.CostEstimate(flops=int(flops), bytes_accessed=int(bytes_accessed), transcendentals=0)


def order_matrix(transposed):
    shape = (128, 112) if transposed else (112, 128)
    row = lax.broadcasted_iota(jnp.int32, shape, 1 if transposed else 0)
    col = lax.broadcasted_iota(jnp.int32, shape, 0 if transposed else 1)
    w_lo, h_hi, w_hi = row // 16, (row // 4) % 4, row % 4
    return (col == h_hi * 32 + w_hi * 7 + w_lo).astype(F32).astype(BF16)


def pair_matrix(first, transposed):
    shape = (224, 224) if transposed else (112, 224)
    row = lax.broadcasted_iota(jnp.int32, shape, 1 if transposed else 0)
    col = lax.broadcasted_iota(jnp.int32, shape, 0 if transposed else 1)
    image = (row // 112 + first) % 2
    row = row % 112
    w_lo, h_hi, w_hi = row // 16, (row // 4) % 4, row % 4
    return (col == h_hi * 56 + (w_hi * 7 + w_lo) * 2 + image).astype(F32).astype(BF16)


def moved(tile, step_h, step_w):
    wide = tile.astype(F32)
    n = wide.shape[1]
    if step_h < 0:
        wide = jnp.concatenate([jnp.zeros((4, n), F32), wide[:12]], axis=0)
    if step_h > 0:
        wide = jnp.concatenate([wide[4:], jnp.zeros((4, n), F32)], axis=0)
    if step_w:
        w_hi = lax.broadcasted_iota(jnp.int32, (GRP, n), 0) % 4
        if step_w < 0:
            wide = jnp.concatenate([wide[15:], wide[:15]], axis=0)
            wide = jnp.where(w_hi == 0, 0.0, wide)
        else:
            wide = jnp.concatenate([wide[1:], wide[:1]], axis=0)
            wide = jnp.where(w_hi == 3, 0.0, wide)
    return wide.astype(BF16)


def fill_halo(dst_ref, value):
    n = value.shape[1]
    groups = value.reshape(LO, LO, GRP, n)
    for a in range(HAL):
        step_h = -1 if a == 0 else (1 if a == HAL - 1 else 0)
        if not step_h:
            dst_ref[a * HAL + 1:a * HAL + 1 + LO] = groups[a - 1]
        for b in range(HAL):
            step_w = -1 if b == 0 else (1 if b == HAL - 1 else 0)
            if step_h or step_w:
                dst_ref[a * HAL + b] = moved(groups[(a - 1) % LO, (b - 1) % LO], step_h, step_w)


def window(ref, i, j):
    parts = [ref[pl.ds((i + a) * HAL + j, LO)] for a in range(LO)]
    whole = jnp.concatenate(parts, axis=0)
    return whole.reshape(PIX, whole.shape[-1])


FWD_FLOPS = 2 * PIX * HALF * CH * 10
W_BYTES = 10 * HALF * CH * 2


def dot_nt(a, b):
    return lax.dot_general(a, b, (((1,), (1,)), ((), ())), preferred_element_type=F32)


def tap_rows(ref, tap):
    last = tap // 9
    base = (1 - last) * ((2 - tap // 3) * HAL + 2 - tap % 3) + last * HAL * HAL
    pitch = HAL - 2 * last
    parts = [ref[pl.ds(base + a * pitch, LO if a < LO - 1 else LO - 1)] for a in range(LO)]
    return jnp.concatenate(parts, axis=0).reshape(MAIN, CH)


def main_kernel(
    act, grad, gam, bet, gms, w_own, s_own,
    x_far, x_diag, x_tails, w_peer, s_peer, vec_out, z_out, z_near, dzm_far, dzm_diag, g_tails, dx_in, sums,
    act_in, pad, xs, xr, xn, xh, im, w_buf, s_buf, pre, short, grad_in, dz_own, dz_send, dz_peer, vec_peer, z_st, dzm_st, g_st, g_near,
    act_sem, x_sem, far_sem, hop_sem, near_sem, diag_sem, w_sem, vec_sem, peer_sem, g_sem, dzm_sem, dx_sem, w_local, keep_sem, tail_sem, out_sem, sum_sem,
):
    t = lax.axis_index("tp")
    stage = lax.axis_index("stage")
    dp = lax.axis_index("dp")

    def act_copy(q):
        col = pl.multiple_of(lax.rem(t * HALF + q * CHUNK, CH), CHUNK)
        return pltpu.make_async_copy(act.at[0, 0, :, :, pl.ds(col, CHUNK)], act_in.at[q], act_sem.at[q])

    grad_copy = pltpu.make_async_copy(grad, grad_in, act_sem.at[4])

    def w_fetch(src_w, src_s, block, q):
        rows = pl.ds(block * CHUNK, CHUNK)
        return (
            pltpu.make_async_copy(src_w.at[:, rows], w_buf.at[q], w_local.at[q, 0]),
            pltpu.make_async_copy(src_s.at[rows], s_buf.at[q], w_local.at[q, 1]),
        )

    @pl.when(stage == 0)
    def _():
        for q in range(N_CHUNKS):
            act_copy(q).start()

    @pl.when(stage == 1)
    def _():
        grad_copy.start()
        for q in range(2):
            for copy in w_fetch(w_own, s_own, q, q):
                copy.start()

    barrier = pltpu.get_barrier_semaphore()
    for target in ({"tp": 1 - t}, {"stage": 1 - stage}, {"dp": 1 - dp}):
        pl.semaphore_signal(barrier, inc=1, device_id=target, device_id_type=MESH)

    def arrange(q):
        select = order_matrix(False)
        act_copy(q).wait()
        pad[:, :SIDE, :] = act_in[q]
        for lo in range(LO):
            rows = jnp.concatenate([pad[hi * LO + lo] for hi in range(4)], axis=0)
            xs[q, lo * 112:(lo + 1) * 112, :] = jnp.dot(select, rows, preferred_element_type=F32).astype(BF16)

    @pl.when(stage == 0)
    def _():
        pad[...] = jnp.zeros_like(pad)
        arrange(0)

    pl.semaphore_wait(barrier, 3)

    def remote(src, dst, sems, target):
        return pltpu.make_async_remote_copy(src_ref=src, dst_ref=dst, send_sem=sems.at[0], recv_sem=sems.at[1], device_id=target, device_id_type=MESH)

    peer, other_stage, other_dp = {"tp": 1 - t}, {"stage": 1 - stage}, {"dp": 1 - dp}

    def x_copy(q):
        return remote(xs.at[q], xr.at[q], x_sem.at[q], other_stage)

    def end_copy(k):
        cols = slice(k * PART, (k + 1) * PART)
        return remote(xs.at[N_CHUNKS - 1, :, cols], xr.at[N_CHUNKS - 1, :, cols], x_sem.at[N_CHUNKS - 1 + k], other_stage)

    def far_copy(q):
        return remote(xs.at[q], xr.at[q], far_sem.at[q], other_dp)

    def hop_copy(q):
        return remote(xr.at[q], x_far.at[q], hop_sem.at[q], other_stage)

    def dx_copy(q):
        return remote(xs.at[q], dx_in.at[q], dx_sem.at[q], other_stage)

    @pl.when(stage == 0)
    def _():
        for q in range(N_CHUNKS):
            if q:
                arrange(q)
            if q < N_CHUNKS - 1:
                x_copy(q).start()
            else:
                end_copy(0).start()
                end_copy(1).start()
            far_copy(q).start()
        for q in range(N_CHUNKS):
            far_copy(q).wait_recv()
            hop_copy(q).start()
        for k in range(2):
            end_copy(k).wait_send()
        for q in range(N_CHUNKS):
            if q < N_CHUNKS - 1:
                x_copy(q).wait_send()
            far_copy(q).wait_send()
            hop_copy(q).wait_send()
        for q in range(N_CHUNKS):
            dx_copy(q).wait_recv()

    @pl.when(stage == 1)
    def _():
        w_copy = remote(w_own, w_peer, w_sem.at[0], peer)
        s_copy = remote(s_own, s_peer, w_sem.at[1], peer)
        vec_copies = [remote(ref, vec_peer.at[k], vec_sem.at[k], peer) for k, ref in enumerate((gam, bet, gms))]
        w_copy.start()
        s_copy.start()
        for copy in vec_copies:
            copy.start()

        grad_copy.wait()
        for image, dst in ((1 - t, dz_send), (t, dz_own)):
            select = pair_matrix(image, False)
            for lo in range(LO):
                rows = jnp.concatenate([grad_in[hi * LO + lo].reshape(56, HALF) for hi in range(4)], axis=0)
                dst[lo * 112:(lo + 1) * 112, :] = jnp.dot(select, rows, preferred_element_type=F32).astype(BF16)
        dz_copy = remote(dz_send, dz_peer, peer_sem.at[0], peer)
        dz_copy.start()

        def near_copy(q):
            return remote(xr.at[q], xn.at[q - 2], near_sem.at[q - 2], peer)

        def land(q, cols):
            n = cols.stop - cols.start
            halo = xh.at[:, :, :n]
            fill_halo(halo, xr[q, :, cols])
            for i in range(3):
                for j in range(3):
                    k = i * 3 + j
                    im[:, k * n:(k + 1) * n] = window(halo, i, j)

        def terms(q, rows, cols):
            k = 9 * (rows.stop - rows.start)
            main = jnp.dot(im[:, :k], w_buf[q, :, rows, cols].reshape(k, HALF), preferred_element_type=F32)
            return main, jnp.dot(xr[q, :, rows], s_buf[q, rows, cols], preferred_element_type=F32)

        whole = slice(0, CHUNK)

        def chunk(q, carry):
            x_copy(q).wait_recv()
            land(q, whole)

            @pl.when(q == 1)
            def _():
                w_copy.wait_recv()
                s_copy.wait_recv()
                for k in range(2):
                    for copy in w_fetch(w_peer, s_peer, k, k + 2):
                        copy.start()

            @pl.when(q == 2)
            def _():
                near_copy(q).start()

            for copy in w_fetch(w_own, s_own, 0, q):
                copy.wait()
            for n in range(2):
                cols = slice(n * HALF, (n + 1) * HALF)
                main, side = terms(q, whole, cols)

                @pl.when(q == 0)
                def _():
                    pre[:, cols] = main
                    short[:, cols] = side

                @pl.when(q > 0)
                def _():
                    pre[:, cols] += main
                    short[:, cols] += side

            return carry

        lax.fori_loop(0, N_CHUNKS - 1, chunk, 0)

        for copy in vec_copies:
            copy.wait_recv()
        dz_copy.wait_recv()

        def dzm_copy(n):
            cols = slice(n * HALF, (n + 1) * HALF)
            return remote(dzm_st.at[:, cols], dzm_far.at[:, cols], dzm_sem.at[n], other_dp)

        def g_copy(n):
            cols = slice(n * HALF, (n + 1) * HALF)
            return remote(g_st.at[:, :, cols], g_near.at[:, :, cols], g_sem.at[n], peer)

        for copy in w_fetch(w_own, s_own, 0, 3):
            copy.wait()
        end_copy(0).wait_recv()
        land(N_CHUNKS - 1, slice(0, PART))
        for n in range(2):
            cols = slice(n * HALF, (n + 1) * HALF)
            main, side = terms(N_CHUNKS - 1, slice(0, PART), cols)
            pre[:, cols] += main
            short[:, cols] += side
        end_copy(1).wait_recv()
        land(N_CHUNKS - 1, slice(PART, CHUNK))
        near_copy(3).start()
        for half in range(2):
            mine = t == half
            main, side = terms(N_CHUNKS - 1, slice(PART, CHUNK), slice(half * HALF, (half + 1) * HALF))
            for n in range(2):
                part = slice(n * TILE, (n + 1) * TILE)
                cols = slice(half * HALF + n * TILE, half * HALF + (n + 1) * TILE)
                gamma, beta, gamma_s = (jnp.where(mine, ref[:, part], vec_peer[k, :, part]) for k, ref in enumerate((gam, bet, gms)))
                for k, row in enumerate((gamma, beta, gamma_s)):
                    vec_out[k:k + 1, cols] = row
                u = (pre[:, cols] + main[:, part]) * gamma + beta + (short[:, cols] + side[:, part]) * gamma_s
                z_st[:, cols] = jnp.maximum(u, 0.0).astype(BF16)
                dz = jnp.where(mine, dz_own[:, part].astype(F32), dz_peer[:, part].astype(F32))
                dz = jnp.where(u > 0.0, dz, 0.0)
                dzm_st[:, cols] = dz.astype(BF16)
                g_st[HAL * HAL:, :, cols] = (dz * gamma_s).astype(BF16).reshape(LO * LO, GRP, TILE)
                fill_halo(g_st.at[:, :, cols], (dz * gamma).astype(BF16))
            dzm_copy(half).start()
            g_copy(half).start()

        mine_at, theirs_at = pl.multiple_of(t * HALF, HALF), pl.multiple_of((1 - t) * HALF, HALF)
        z_copy = remote(z_st.at[:, pl.ds(theirs_at, HALF)], z_near, peer_sem.at[2], peer)
        z_keep = pltpu.make_async_copy(z_st.at[:, pl.ds(mine_at, HALF)], z_out, keep_sem)
        z_copy.start()
        z_keep.start()

        def dx_chunk(q, carry):
            total = dot_nt(g_st[HAL * HAL:].reshape(PIX, CH), s_buf[q])
            for k in range(9):
                total = total + dot_nt(window(g_st, 2 - k // 3, 2 - k % 3), w_buf[q, k])
            xs[q] = total.astype(BF16)
            dx_copy(q).start()
            return carry

        lax.fori_loop(0, N_CHUNKS, dx_chunk, 0)

        near_copy(2).wait_recv()
        near_copy(3).wait_recv()
        g_copy(0).wait_recv()
        g_copy(1).wait_recv()
        tails = []
        for k, (x_ref, g_ref) in enumerate(((xr, g_st), (xn, g_near))):
            tails.append(pltpu.make_async_copy(x_ref.at[0:2, MAIN:PIX], x_tails.at[k], tail_sem.at[k, 0]))
            for i in range(3):
                at = (LO - 1 + i) * HAL + LO - 1
                tails.append(pltpu.make_async_copy(g_ref.at[at:at + 3], g_tails.at[k, 3 * i:3 * i + 3], tail_sem.at[k, 1 + i]))
            tails.append(pltpu.make_async_copy(g_ref.at[GROUPS - 1:GROUPS], g_tails.at[k, 9:10], tail_sem.at[k, 4]))
        for copy in tails:
            copy.start()
        for q in range(2):
            rows = slice(q * CHUNK, (q + 1) * CHUNK)
            im[rows, :MAIN] = xr[q, :MAIN, :].T
            im[rows, MAIN:2 * MAIN] = xn[q, :MAIN, :].T

        def diag_copy(k):
            return remote(x_far.at[2 + k], x_diag.at[k], diag_sem.at[k], peer)

        def dzm_diag_copy(n):
            cols = slice(n * HALF, (n + 1) * HALF)
            return remote(dzm_far.at[:, cols], dzm_diag.at[:, cols], dzm_sem.at[2 + n], peer)

        def sum_copy(tap, k):
            return pltpu.make_async_copy((pre, short)[k].at[:HALF], sums.at[tap], sum_sem.at[k])

        def sum_pair(p, carry):
            @pl.when(p == 4)
            def _():
                for k in range(2):
                    hop_copy(2 + k).wait_recv()
                    diag_copy(k).start()

            for n in range(2):
                @pl.when(p == 3 + n)
                def _():
                    dzm_copy(n).wait_recv()
                    dzm_diag_copy(n).start()

            for k in range(2):
                tap = 2 * p + k
                rows = jnp.concatenate([tap_rows(g_st, tap), tap_rows(g_near, tap)], axis=0)
                total = jnp.dot(im[:HALF, :2 * MAIN], rows, preferred_element_type=F32)

                @pl.when(p > 0)
                def _():
                    sum_copy(tap - 2, k).wait()

                (pre, short)[k][:HALF] = total
                sum_copy(tap, k).start()
            return carry

        lax.fori_loop(0, 5, sum_pair, 0)

        for k in range(2):
            sum_copy(8 + k, k).wait()
            hop_copy(k).wait_recv()
            near_copy(2 + k).wait_send()
            diag_copy(k).wait()
        for q in range(N_CHUNKS):
            dx_copy(q).wait_send()
        for copy in tails:
            copy.wait()
        z_keep.wait()
        z_copy.wait()
        for n in range(2):
            dzm_diag_copy(n).wait()
        for copy in [w_copy, s_copy, dz_copy, dzm_copy(0), dzm_copy(1), g_copy(0), g_copy(1)] + vec_copies:
            copy.wait_send()


def main(act_in, grad_z, gamma, beta, gamma_s, w_own, s_own):
    vmem = pl.BlockSpec(memory_space=pltpu.VMEM)
    anywhere = pl.BlockSpec(memory_space=pl.ANY)
    dma = pltpu.SemaphoreType.DMA
    chunks = (N_CHUNKS, PIX, CHUNK)
    return pl.pallas_call(
        main_kernel,
        in_specs=[anywhere] * 2 + [vmem] * 3 + [anywhere] * 2,
        out_specs=[anywhere] * 5 + [vmem] + [anywhere] * 7,
        out_shape=[
            jax.ShapeDtypeStruct(chunks, BF16),
            jax.ShapeDtypeStruct((2, PIX, CHUNK), BF16),
            jax.ShapeDtypeStruct((2, 2, GRP, CHUNK), BF16),
            jax.ShapeDtypeStruct((9, HALF, CH), BF16),
            jax.ShapeDtypeStruct((HALF, CH), BF16),
            jax.ShapeDtypeStruct((3, CH), F32),
            jax.ShapeDtypeStruct((PIX, HALF), BF16),
            jax.ShapeDtypeStruct((PIX, HALF), BF16),
            jax.ShapeDtypeStruct((PIX, CH), BF16),
            jax.ShapeDtypeStruct((PIX, CH), BF16),
            jax.ShapeDtypeStruct((2, 10, GRP, CH), BF16),
            jax.ShapeDtypeStruct(chunks, BF16),
            jax.ShapeDtypeStruct((10, HALF, CH), F32),
        ],
        scratch_shapes=[
            pltpu.VMEM((N_CHUNKS, SIDE, SIDE, CHUNK), BF16),
            pltpu.VMEM((SIDE, 32, CHUNK), BF16),
            pltpu.VMEM(chunks, BF16),
            pltpu.VMEM(chunks, BF16),
            pltpu.VMEM((2, PIX, CHUNK), BF16),
            pltpu.VMEM((HAL * HAL, GRP, CHUNK), BF16),
            pltpu.VMEM((PIX, 9 * CHUNK), BF16),
            pltpu.VMEM((N_CHUNKS, 9, CHUNK, CH), BF16),
            pltpu.VMEM((N_CHUNKS, CHUNK, CH), BF16),
            pltpu.VMEM((PIX, CH), F32),
            pltpu.VMEM((PIX, CH), F32),
            pltpu.VMEM((SIDE, SIDE, 2, HALF), BF16),
            pltpu.VMEM((PIX, HALF), BF16),
            pltpu.VMEM((PIX, HALF), BF16),
            pltpu.VMEM((PIX, HALF), BF16),
            pltpu.VMEM((3, 1, HALF), F32),
            pltpu.VMEM((PIX, CH), BF16),
            pltpu.VMEM((PIX, CH), BF16),
            pltpu.VMEM((GROUPS, GRP, CH), BF16),
            pltpu.VMEM((GROUPS, GRP, CH), BF16),
            dma((5,)), dma((5, 2)), dma((4, 2)), dma((4, 2)), dma((2, 2)), dma((2, 2)), dma((2, 2)), dma((3, 2)), dma((3, 2)), dma((2, 2)), dma((4, 2)),
            dma((4, 2)), dma((4, 2)), dma, dma((2, 5)), dma, dma((2,)),
        ],
        compiler_params=pltpu.CompilerParams(collective_id=0, has_side_effects=True, vmem_limit_bytes=66 * 1000 * 1000),
        cost_estimate=cost(6 * FWD_FLOPS, 2 * W_BYTES),
        name="main",
    )(act_in, jnp.transpose(grad_z[0], (1, 2, 0, 3)), gamma, beta, gamma_s, w_own, s_own)


SLOTS = 4


def last_kernel(
    xa, xb, x_ends, dza, dzb, vec, g_ends, sums, z, z_near, dx,
    dw_out, ds_out, z_out, dx_out,
    xa_v, xb_v, dza_v, dzb_v, x_tails, vec_ref, g_tails, sum_v, tot_v, z_v, zn_v, dx_v, z_st, dx_st, ga_ref, gb_ref, gsa_ref, gsb_ref, xt_ref, in_sem, small_sem, sum_sem, tot_sem, side_sem, out_sem,
):
    step = pl.program_id(0)
    t = lax.axis_index("tp")
    stage = lax.axis_index("stage")
    fetches = [
        pltpu.make_async_copy(src, dst, in_sem.at[k])
        for k, (src, dst) in enumerate(((xa.at[0:2], xa_v), (dza, dza_v), (xb, xb_v), (dzb, dzb_v)))
    ]
    smalls = [pltpu.make_async_copy(src, dst, small_sem.at[k]) for k, (src, dst) in enumerate(((vec, vec_ref), (x_ends, x_tails), (g_ends, g_tails)))]
    sides = [pltpu.make_async_copy(src, dst, side_sem.at[k]) for k, (src, dst) in enumerate(((z, z_v), (z_near, zn_v), (dx, dx_v)))]
    outs = [pltpu.make_async_copy(src, dst, out_sem.at[k]) for k, (src, dst) in enumerate(((z_st, z_out), (dx_st, dx_out)))]

    def sum_fetch(term):
        return pltpu.make_async_copy(sums.at[(term + 9) % 10], sum_v.at[term % SLOTS], sum_sem.at[term % SLOTS])

    def tot_copy(term):
        tap = term - 1
        return pltpu.make_async_copy(tot_v.at[term % SLOTS], dw_out.at[0, tap // 3, tap % 3], tot_sem.at[term % SLOTS])

    short_copy = pltpu.make_async_copy(tot_v.at[0], ds_out.at[0], tot_sem.at[0])

    def product(parts):
        return jnp.dot(xt_ref[...], jnp.concatenate(parts, axis=0), preferred_element_type=F32)

    def tap_product(tap):
        i, j = 2 - tap // 3, 2 - tap % 3
        final = (LO - 1 + i) * HAL + LO - 1 + j
        end = i * 3 + j
        return product([tap_rows(ga_ref, tap), tap_rows(gb_ref, tap), ga_ref[final], gb_ref[final], g_tails[0, end], g_tails[1, end]])

    @pl.when((step == 0) & (stage == 1))
    def _():
        images = ((xa_v, dza_v, ga_ref, gsa_ref), (xb_v, dzb_v, gb_ref, gsb_ref))
        for copy in [smalls[0]] + fetches + smalls[1:]:
            copy.start()
        smalls[0].wait()
        for k, (x_v, dz_v, g_ref, gs_ref) in enumerate(images):
            fetches[2 * k].wait()
            for q in range(2):
                rows = slice(q * CHUNK, (q + 1) * CHUNK)
                xt_ref[rows, k * MAIN:(k + 1) * MAIN] = x_v[q, :MAIN, :].T
            fetches[2 * k + 1].wait()
            if k == 1:
                sum_fetch(0).start()
                sum_fetch(1).start()
            gs_ref[...] = (dz_v[...].astype(F32) * vec_ref[2:3, :]).astype(BF16)
            if k == 0:
                tot_v[0] = jnp.dot(xt_ref[:, :MAIN], gsa_ref[:MAIN], preferred_element_type=F32)
        for copy in smalls[1:]:
            copy.wait()
        for q in range(2):
            rows = slice(q * CHUNK, (q + 1) * CHUNK)
            ends = [xa_v[q, MAIN:, :], xb_v[q, MAIN:, :], x_tails[0, q], x_tails[1, q]]
            xt_ref[rows, 2 * MAIN:] = jnp.concatenate(ends, axis=0).T
        rest = jnp.concatenate([gsb_ref[:MAIN], gsa_ref[MAIN:], gsb_ref[MAIN:], g_tails[0, 9], g_tails[1, 9]], axis=0)
        total = jnp.dot(xt_ref[:, MAIN:], rest, preferred_element_type=F32)
        for x_v, dz_v, g_ref, gs_ref in images:
            for n in range(CH // TILE):
                cols = slice(n * TILE, (n + 1) * TILE)
                fill_halo(g_ref.at[:, :, cols], (dz_v[:, cols].astype(F32) * vec_ref[0:1, cols]).astype(BF16))
        for copy in sides[:2]:
            copy.start()
        sum_fetch(2).start()
        sum_fetch(3).start()
        sum_fetch(0).wait()
        tot_v[0] += total + sum_v[0]
        short_copy.start()
        sum_fetch(1).wait()
        tot_v[1] = tap_product(0) + sum_v[1]
        tot_copy(1).start()

    def drain(term):
        @pl.when(term == 4)
        def _():
            short_copy.wait()

        @pl.when(term != 4)
        def _():
            tot_copy(term - SLOTS).wait()

    @pl.when((step > 0) & (stage == 1))
    def _():
        @pl.when(step < 4)
        def _():
            sum_fetch(2 * step + 2).start()
            sum_fetch(2 * step + 3).start()

        @pl.when(step > 1)
        def _():
            drain(2 * step)
            drain(2 * step + 1)

        sum_fetch(2 * step).wait()
        sum_fetch(2 * step + 1).wait()
        for k in range(2):
            term = 2 * step + k
            tot_v[term % SLOTS] = tap_product(term - 1) + sum_v[term % SLOTS]
            tot_copy(term).start()

    @pl.when((step == 0) & (stage == 0))
    def _():
        sides[2].start()
        z_st[...] = jnp.zeros_like(z_st)
        outs[0].start()
        tot_v[0] = jnp.zeros_like(tot_v[0])
        short_copy.start()
        short_copy.wait()
        sides[2].wait()
        select = order_matrix(True)
        for lo in range(LO):
            for q in range(N_CHUNKS):
                to = pl.multiple_of(lax.rem(t * HALF + q * CHUNK, CH), CHUNK)
                rows = jnp.dot(select, dx_v[q, lo * 112:(lo + 1) * 112, :], preferred_element_type=F32).astype(BF16)
                for hi in range(4):
                    dx_st[0, 0, hi * LO + lo, :, pl.ds(to, CHUNK)] = rows[hi * 32:hi * 32 + SIDE, :]
        outs[1].start()

        def clear(tap, carry):
            copy = pltpu.make_async_copy(tot_v.at[0], dw_out.at[0, tap // 3, tap % 3], tot_sem.at[0])
            copy.start()
            copy.wait()
            return carry

        lax.fori_loop(0, 9, clear, 0)

    @pl.when((step == 1) & (stage == 1))
    def _():
        dx_st[...] = jnp.zeros_like(dx_st)
        outs[1].start()
        for copy in sides[:2]:
            copy.wait()
        select = pair_matrix(t, True)
        for lo in range(LO):
            part = slice(lo * 112, (lo + 1) * 112)
            both = jnp.concatenate([z_v[part, :], zn_v[part, :]], axis=0)
            rows = jnp.dot(select, both, preferred_element_type=F32)
            for hi in range(4):
                z_st[hi * LO + lo] = rows[hi * 56:(hi + 1) * 56].astype(BF16).reshape(SIDE, 2, HALF)
        outs[0].start()

    @pl.when(step == 4)
    def _():
        for copy in outs:
            copy.wait()

    @pl.when((step == 4) & (stage == 1))
    def _():
        for term in range(6, 10):
            tot_copy(term).wait()


def last(x_far, x_diag, x_tails, dzm_far, dzm_diag, vec, g_tails, sums, z, z_near, dx):
    anywhere = pl.BlockSpec(memory_space=pl.ANY)
    dma = pltpu.SemaphoreType.DMA
    z_shape, dx_shape = (SIDE, SIDE, 2, HALF), (1, 1, SIDE, SIDE, CH)
    dw, ds, z_out, dx_out = pl.pallas_call(
        last_kernel,
        grid=(5,),
        in_specs=[anywhere] * 11,
        out_specs=[anywhere] * 4,
        out_shape=[
            jax.ShapeDtypeStruct((1, 3, 3, HALF, CH), F32),
            jax.ShapeDtypeStruct((1, HALF, CH), F32),
            jax.ShapeDtypeStruct(z_shape, BF16),
            jax.ShapeDtypeStruct(dx_shape, BF16),
        ],
        scratch_shapes=[
            pltpu.VMEM((2, PIX, CHUNK), BF16),
            pltpu.VMEM((2, PIX, CHUNK), BF16),
            pltpu.VMEM((PIX, CH), BF16),
            pltpu.VMEM((PIX, CH), BF16),
            pltpu.VMEM((2, 2, GRP, CHUNK), BF16),
            pltpu.VMEM((3, CH), F32),
            pltpu.VMEM((2, 10, GRP, CH), BF16),
            pltpu.VMEM((SLOTS, HALF, CH), F32),
            pltpu.VMEM((SLOTS, HALF, CH), F32),
            pltpu.VMEM((PIX, HALF), BF16),
            pltpu.VMEM((PIX, HALF), BF16),
            pltpu.VMEM((N_CHUNKS, PIX, CHUNK), BF16),
            pltpu.VMEM(z_shape, BF16),
            pltpu.VMEM(dx_shape, BF16),
            pltpu.VMEM((HAL * HAL, GRP, CH), BF16),
            pltpu.VMEM((HAL * HAL, GRP, CH), BF16),
            pltpu.VMEM((PIX, CH), BF16),
            pltpu.VMEM((PIX, CH), BF16),
            pltpu.VMEM((HALF, 2 * PIX + 2 * GRP), BF16),
            dma((4,)), dma((3,)), dma((SLOTS,)), dma((SLOTS,)), dma((3,)), dma((2,)),
        ],
        compiler_params=params(1),
        cost_estimate=cost(2 * FWD_FLOPS, 2 * W_BYTES),
        name="last",
    )(x_far, x_diag, x_tails, dzm_far, dzm_diag, vec, g_tails, sums, z, z_near, dx)
    return jnp.transpose(z_out, (2, 0, 1, 3))[None], dx_out, dw, ds


def solution(mesh):
    act_spec = P("stage", ("dp", "tp"), None, None, None)
    kernel_spec = P("stage", None, None, "tp", None)
    short_spec = P("stage", "tp", None)
    vec_spec = P("stage", "tp")
    grad_spec = P("stage", "dp", None, None, "tp")

    def device_step(act_in, w_conv, w_short, gamma, beta, gamma_s, grad_z):
        w_own = w_conv.reshape(9, HALF, CH)
        s_own = w_short.reshape(HALF, CH)
        x_far, x_diag, x_tails, _, _, vec, z, z_near, dzm_far, dzm_diag, g_tails, dx, sums = main(act_in, grad_z, gamma, beta, gamma_s, w_own, s_own)
        return last(x_far, x_diag, x_tails, dzm_far, dzm_diag, vec, g_tails, sums, z, z_near, dx)

    return jax.shard_map(device_step, mesh=mesh, in_specs=(act_spec, kernel_spec, short_spec, vec_spec, vec_spec, vec_spec, grad_spec), out_specs=(grad_spec, act_spec, kernel_spec, short_spec), check_vma=False)
```
